512 devices in a mesh: groups: 2 (over y), ctx: 32 (over z), rep: 4 (over x), row: 2 (over core).
Axes of the slice: x: 4, y: 2, z: 32, core: 2. Of those that a mesh axis runs over, the one named last changes fastest.
The devices are a block of a 4x8x32 slice.
Arguments:
- queries: bfloat16 [4, 128, 64, 128], P(None, ('groups', 'ctx', 'row'), 'rep'), parts along dimension 1, may hold values from -8 to 8
- new_keys: bfloat16 [4, 128, 8, 128], P(None, ('groups', 'ctx', 'row'), 'rep'), parts along dimension 1, may hold values from -4.5 to 4.5
- step_new_values: bfloat16 [4, 128, 8, 128], P(None, ('groups', 'ctx', 'row'), 'rep'), parts along dimension 1, may hold values from -6 to 6
- context_keys: bfloat16 [8, 32768, 128], P('rep', ('groups', 'ctx')), parts along dimension 1, may hold values from -6 to 6
- context_values: bfloat16 [8, 32768, 128], P('rep', ('groups', 'ctx')), parts along dimension 1, may hold values from -6 to 6
- cluster_centroid_keys: bfloat16 [8, 256, 128], P('rep', ('groups', 'ctx')), parts along dimension 1, may hold values from -4 to 4
- cluster_mean_values: bfloat16 [8, 256, 128], P('rep', ('groups', 'ctx')), parts along dimension 1, may hold values from -6 to 6
- cluster_page_slot: int32 [8, 256], P('rep', 'groups'), parts along dimension 1, may hold values from 0 to 127, each once within a row
- picks: int32 [128, 8, 16], P(('groups', 'ctx', 'row'), 'rep'), parts along dimension 0, may hold values from 0 to 127, all different within a row
Outputs:
- attention: bfloat16 [4, 128, 64, 128], P(None, ('groups', 'ctx', 'row'), 'rep'), parts along dimension 1
The draws below stay inside these ranges and needn't reach their ends.
There are 2 independent parts, one for each index of `groups`. The reference program is written for one: setup_inputs(seed, part) draws one part's arguments, and reference() takes and returns one part's arrays. A program takes and returns all parts, laid end to end along the dimension named above; each array names one. Nothing has to cross between parts.
Inputs may be any that keep to these rules, and one draw needn't show every extreme that they name: `picks`: for each row and key-value head, 16 different cluster ids. `cluster_page_slot`: for each key-value head, every cluster has its own page slot; slot p lies on context shard p // 4.
All inputs are finite; a program needn't handle non-finite values.
Results may differ from the reference program's by a relative error of at most 0.0027.
Values may be sent and summed in bfloat16 or wider, within the bound.
No kernel may reach another device: no remote copies, remote signals or barrier semaphores. Data moves between devices by JAX's collectives and lax.ppermute only.
A program may use at most 64 MiB of HBM per device.

```python
import math
import jax
import jax.numpy as jnp
from jax import lax

QUERY_HEADS = 64
KEY_VALUE_HEADS = 8
HEAD_SIZE = 128
SPAN_PER_GROUPING = 128
PICKED_CLUSTERS = 16
DECODE_STEPS = 4
CL_DEV = 4
DECODE_ROWS = 64
CLUSTER_COUNT = 128
CONTEXT_LENGTH = 16384
N_CTX = 32


def draw_queries(key, part):
    base_offset = jax.random.fold_in(key, 3)
    value_rows = 2.0 * jax.random.truncated_normal(base_offset, -4.0, 4.0, (DECODE_STEPS, DECODE_ROWS, QUERY_HEADS, HEAD_SIZE), jnp.float32)
    return value_rows.astype(jnp.bfloat16)


def draw_new_keys(key, part):
    base_offset = jax.random.fold_in(key, 5)
    value_rows = jax.random.truncated_normal(base_offset, -4.5, 4.5, (DECODE_STEPS, DECODE_ROWS, KEY_VALUE_HEADS, HEAD_SIZE), jnp.float32)
    return value_rows.astype(jnp.bfloat16)


def draw_context_keys(key, part):
    base_offset = jax.random.fold_in(key, 7)
    value_rows = jax.random.truncated_normal(base_offset, -6.0, 6.0, (KEY_VALUE_HEADS, CONTEXT_LENGTH, HEAD_SIZE), jnp.float32)
    return value_rows.astype(jnp.bfloat16)


def block_levels(stream_key, shape, pieces, low, high):
    factor_of, own = 1.0, jax.random.fold_in(stream_key, 6)
    for axis_at, blocks in pieces:
        steps = jnp.exp(jax.random.uniform(jax.random.fold_in(own, axis_at), (blocks,), jnp.float32, low / len(pieces), high / len(pieces)))
        factor_of = factor_of * jnp.repeat(steps, shape[axis_at] // blocks).reshape([-1 if axis == axis_at else 1 for axis in range(len(shape))])
    return factor_of


def distinct(key, rows, number_of, top, lift):
    ranking = jax.random.permutation(jax.random.fold_in(key, 1), number_of)
    boost = ranking
    for power in range(3):
        boost = boost * boost // number_of
    boost = boost * lift // number_of
    lots = jax.random.randint(jax.random.fold_in(key, 2), (rows, number_of), 0, 4096) + boost
    holders = jax.random.permutation(jax.random.fold_in(key, 3), rows)[jnp.arange(number_of) % rows]
    lots = jnp.where(jnp.arange(rows)[:, None] == holders[None, :], 1 << 14, lots)
    merit = lots * number_of + jnp.arange(number_of)
    return lax.top_k(merit.astype(jnp.int32), top)[1].astype(jnp.int32)


def scatter_about(rng, extent, scale, reach, shards=(), kind=jnp.bfloat16):
    level = block_levels(rng, extent, shards, -0.22, 0.18) if shards else 1.0
    values = jax.random.normal(rng, extent, jnp.float32) * scale * level
    return jnp.minimum(jnp.maximum(values, -reach), reach).astype(kind)


def setup_inputs(seed: int = 0, part: int = 0) -> dict:
    key_list = jax.random.split(jax.random.key(seed), 10)
    part_splits = jax.random.split(jax.random.fold_in(key_list[9], part), 10)
    return {
        "queries": draw_queries(jax.random.fold_in(jax.random.fold_in(key_list[9], part), 71), part),
        "new_keys": draw_new_keys(jax.random.fold_in(jax.random.fold_in(key_list[9], part), 71), part),
        "step_new_values": scatter_about(part_splits[2], (DECODE_STEPS, DECODE_ROWS, KEY_VALUE_HEADS, HEAD_SIZE), 1.0, 6.0, ((1, 64), (2, 4))),
        "context_keys": draw_context_keys(jax.random.fold_in(jax.random.fold_in(key_list[9], part), 71), part),
        "context_values": scatter_about(part_splits[4], (KEY_VALUE_HEADS, CONTEXT_LENGTH, HEAD_SIZE), 1.0, 6.0, ((0, 4), (1, 32))),
        "cluster_centroid_keys": scatter_about(part_splits[5], (KEY_VALUE_HEADS, CLUSTER_COUNT, HEAD_SIZE), 0.6, 4.0, ((0, 4), (1, 32))),
        "cluster_mean_values": scatter_about(part_splits[6], (KEY_VALUE_HEADS, CLUSTER_COUNT, HEAD_SIZE), 1.0, 6.0, ((0, 4), (1, 32))),
        "cluster_page_slot": jax.vmap(lambda own: jax.random.permutation(own, CLUSTER_COUNT))(jax.random.split(part_splits[7], KEY_VALUE_HEADS)).reshape((KEY_VALUE_HEADS, CLUSTER_COUNT)).astype(jnp.int32),
        "picks": distinct(part_splits[8], DECODE_ROWS * KEY_VALUE_HEADS, CLUSTER_COUNT, PICKED_CLUSTERS, 2048).reshape((DECODE_ROWS, KEY_VALUE_HEADS, PICKED_CLUSTERS)),
    }


FLOOR_SCORE = -10000.0

def tail_block(queries, new_keys, step_new_values, logit_multiplier):
    num_steps, num_rows, num_heads, head_width = queries.shape
    kv_heads = new_keys.shape[2]
    grouped = queries.astype(jnp.float32).reshape(num_steps, num_rows, kv_heads, num_heads // kv_heads, head_width)
    scores = jnp.einsum('srhgd,trhd->srhgt', grouped, new_keys.astype(jnp.float32)) * logit_multiplier
    step_ids = jnp.arange(num_steps, dtype=jnp.int32)
    causal = (step_ids[None, :] <= step_ids[:, None])[:, None, None, None, :]
    block_top = lax.optimization_barrier(jnp.max(jnp.where(causal, scores, FLOOR_SCORE), axis=-1))
    weights = jnp.where(causal, jnp.exp(scores - block_top[..., None]), 0.0)
    sum_total = lax.optimization_barrier(jnp.sum(weights, axis=-1))
    rounded = weights.astype(jnp.bfloat16).astype(jnp.float32)
    tail_out = jnp.einsum('srhgt,trhd->srhgd', rounded, step_new_values.astype(jnp.float32))
    return (tail_out.reshape(num_steps, num_rows, num_heads, head_width), sum_total.reshape(num_steps, num_rows, num_heads), block_top.reshape(num_steps, num_rows, num_heads))

def reference(queries, new_keys, step_new_values, context_keys, context_values, cluster_centroid_keys, cluster_mean_values, cluster_page_slot, picks):
    logit_multiplier = 1.0 / math.sqrt(HEAD_SIZE)
    membership_log_weight = math.log(SPAN_PER_GROUPING)
    query_group_size = QUERY_HEADS // KEY_VALUE_HEADS
    span_tokens = CL_DEV * SPAN_PER_GROUPING
    cluster_ids = jnp.arange(CLUSTER_COUNT, dtype=jnp.int32)
    chosen_page_slot = jnp.take_along_axis(jnp.broadcast_to(cluster_page_slot[None], (DECODE_ROWS, KEY_VALUE_HEADS, CLUSTER_COUNT)), picks, axis=2)
    slot_used = jnp.any(chosen_page_slot[..., None] == cluster_ids, axis=2)
    cluster_used = jnp.any(picks[..., None] == cluster_ids, axis=2)
    tail_out, tail_total, tail_top = tail_block(queries, new_keys, step_new_values, logit_multiplier)
    results = []
    for step_index in range(DECODE_STEPS):
        head_outs, head_totals, head_tops = ([], [], [])
        for current_head_index in range(KEY_VALUE_HEADS):
            generation_probe_vectors = queries[step_index, :, current_head_index * query_group_size:(current_head_index + 1) * query_group_size, :].reshape(DECODE_ROWS * query_group_size, HEAD_SIZE)
            head_keys = context_keys[current_head_index]
            head_values = context_values[current_head_index]
            head_cents = cluster_centroid_keys[current_head_index]
            head_cvals = cluster_mean_values[current_head_index]
            head_slots = slot_used[:, current_head_index]
            head_clusters = cluster_used[:, current_head_index]

            def block_part(shard_index):
                first_token = (shard_index * span_tokens).astype(jnp.int32)
                first_cluster = (shard_index * CL_DEV).astype(jnp.int32)
                block_keys = lax.dynamic_slice_in_dim(head_keys, first_token, span_tokens, 0)
                block_values = lax.dynamic_slice_in_dim(head_values, first_token, span_tokens, 0)
                tile_prototype_vectors = lax.dynamic_slice_in_dim(head_cents, first_cluster, CL_DEV, 0)
                block_cvals = lax.dynamic_slice_in_dim(head_cvals, first_cluster, CL_DEV, 0)
                exact_mask = lax.dynamic_slice_in_dim(head_slots, first_cluster, CL_DEV, 1)[:, None, :, None]
                coarse_mask = jnp.logical_not(lax.dynamic_slice_in_dim(head_clusters, first_cluster, CL_DEV, 1))[:, None, :]
                exact_scores = jnp.dot(generation_probe_vectors, block_keys.T, preferred_element_type=jnp.float32) * logit_multiplier
                exact_scores = exact_scores.reshape(DECODE_ROWS, query_group_size, CL_DEV, SPAN_PER_GROUPING)
                prototype_logits = jnp.dot(generation_probe_vectors, tile_prototype_vectors.T, preferred_element_type=jnp.float32) * logit_multiplier + membership_log_weight
                prototype_logits = prototype_logits.reshape(DECODE_ROWS, query_group_size, CL_DEV)
                block_top = jnp.maximum(lax.optimization_barrier(jnp.max(jnp.where(exact_mask, exact_scores, FLOOR_SCORE), axis=(2, 3))), lax.optimization_barrier(jnp.max(jnp.where(coarse_mask, prototype_logits, FLOOR_SCORE), axis=2)))
                exact_weights = jnp.where(exact_mask, jnp.exp(exact_scores - block_top[:, :, None, None]), 0.0)
                coarse_weights = jnp.where(coarse_mask, jnp.exp(prototype_logits - block_top[:, :, None]), 0.0)
                sum_total = lax.optimization_barrier(jnp.sum(exact_weights, axis=(2, 3))) + lax.optimization_barrier(jnp.sum(coarse_weights, axis=2))
                block_out = jnp.dot(exact_weights.astype(jnp.bfloat16).reshape(DECODE_ROWS * query_group_size, span_tokens), block_values, preferred_element_type=jnp.float32)
                block_out = block_out + jnp.dot(coarse_weights.astype(jnp.bfloat16).reshape(DECODE_ROWS * query_group_size, CL_DEV), block_cvals, preferred_element_type=jnp.float32)
                return (block_out.reshape(DECODE_ROWS, query_group_size, HEAD_SIZE), sum_total, block_top)
            partial_outs, partial_totals, partial_tops = lax.map(block_part, jnp.arange(N_CTX, dtype=jnp.int32))
            best_top = lax.optimization_barrier(jnp.max(partial_tops, axis=0))
            factor = jnp.exp(partial_tops - best_top)
            head_outs.append(lax.optimization_barrier(jnp.sum(factor[..., None] * partial_outs, axis=0)))
            head_totals.append(lax.optimization_barrier(jnp.sum(factor * partial_totals, axis=0)))
            head_tops.append(best_top)
        merged = jnp.concatenate(head_outs, axis=1)
        sum_total = jnp.concatenate(head_totals, axis=1)
        best_top = jnp.concatenate(head_tops, axis=1)
        overall = jnp.maximum(best_top, tail_top[step_index])
        context_factor = jnp.exp(best_top - overall)
        tail_factor = jnp.exp(tail_top[step_index] - overall)
        numer = context_factor[..., None] * merged + tail_factor[..., None] * tail_out[step_index]
        denom = context_factor * sum_total + tail_factor * tail_total[step_index]
        results.append(numer / denom[..., None])
    return jnp.stack(results).astype(jnp.bfloat16)
```

```python
import functools
import math

import jax
import jax.numpy as jnp
from jax import lax
from jax.experimental import pallas as pl
from jax.experimental.pallas import tpu as pltpu
from jax.sharding import PartitionSpec as P

FLOOR_SCORE = -10000.0
MASKED = -(2.0**100)
NEAR = 4
RING = ("hi", "lo")
PEERS = ("hi", "row")
LANES = 128


def place():
    return lax.axis_index("hi") * NEAR + lax.axis_index("lo"), lax.axis_index("row")


def near_offsets(core):
    return (0, 1, -1, 2 - 4 * core)


def prepare(heads, clusters, picks_ref, slots_ref, q_ref, k_ref, v_ref, ck_ref, cv_ref, ask_ref, pages_ref):
    num_steps, _, num_heads, width = q_ref.shape
    group = num_heads // heads
    peers = ask_ref.shape[0]
    cores = heads
    lane = lax.broadcasted_iota(jnp.int32, (8, width), 1)
    sub = lax.broadcasted_iota(jnp.int32, (8, width), 0)
    for head in range(heads):
        slot_free = jnp.ones((8, width), jnp.float32)
        cluster_used = jnp.zeros((8, width), jnp.float32)
        for i in range(picks_ref.shape[2]):
            pick = picks_ref[0, head, i]
            slot_free = jnp.where(lane == slots_ref[head, pick], 0.0, slot_free)
            cluster_used = jnp.where(lane == pick, 1.0, cluster_used)
        masks = jnp.where(sub == 0, slot_free, jnp.where(sub == 1, cluster_used, 0.0))
        rows = [
            q_ref[s, 0, head * group : (head + 1) * group, :].astype(jnp.float32)
            for s in range(num_steps)
        ]
        message = jnp.concatenate(rows + [masks], axis=0).astype(ask_ref.dtype)
        for hi in range(peers // cores):
            ask_ref[hi * cores + head] = message
    core = lax.axis_index("row")
    span = k_ref.shape[1]
    near = ck_ref.shape[1]
    pages_ref[0:span, :] = k_ref[core]
    pages_ref[span : 2 * span, :] = v_ref[core]
    coarse = jnp.concatenate(
        [ck_ref[core].astype(jnp.float32), cv_ref[core].astype(jnp.float32)]
        + [jnp.zeros((16 - 2 * near, width), jnp.float32)],
        axis=0,
    )
    pages_ref[2 * span :, :] = coarse.astype(pages_ref.dtype)


def attend(span, near, ring, ask_ref, *rest):
    page_refs, reply_ref = rest[:NEAR], rest[NEAR]
    peers, height, width = ask_ref.shape
    per_peer = height - 8
    scale = 1.0 / math.sqrt(width)
    log_page = math.log(span // near)
    chunk_peers = LANES // per_peer
    position, core = place()
    shards = [lax.rem(position + off + ring, ring) for off in near_offsets(core)]
    page = span // near
    lane = lax.broadcasted_iota(jnp.int32, (page, width), 1)
    keys = []
    for ref, shard in zip(page_refs, shards):
        picker = jnp.concatenate(
            [jnp.where(lane == shard * near + p, MASKED, 0.0) for p in range(near)], axis=0
        ).astype(jnp.bfloat16)
        keys.append(jnp.concatenate([ref[0:span, :], picker], axis=1))
    ends = [ref[2 * span :, :].astype(jnp.float32) for ref in page_refs]
    blank = jnp.zeros((LANES - near * NEAR, width), jnp.float32)
    coarse_keys = jnp.concatenate([e[0:near] for e in ends] + [blank], axis=0)
    coarse_values = jnp.concatenate([e[near : 2 * near] for e in ends] + [blank], axis=0)
    coarse_values = coarse_values.astype(jnp.bfloat16)
    row = lax.broadcasted_iota(jnp.int32, (LANES, width), 0)
    column = lax.broadcasted_iota(jnp.int32, (LANES, width), 1)
    cluster = jnp.full((LANES, width), -1, jnp.int32)
    for b, shard in enumerate(shards):
        cluster = jnp.where(row // near == b, shard * near + row - b * near, cluster)
    picker = jnp.where(column == cluster, MASKED, 0.0)
    coarse_keys = jnp.concatenate([coarse_keys, picker], axis=1).astype(jnp.bfloat16)
    block_of = lax.broadcasted_iota(jnp.int32, (LANES, LANES), 1) // near
    lane8 = lax.broadcasted_iota(jnp.int32, (LANES, LANES), 1)
    contract_last = (((1,), (1,)), ((), ()))

    for chunk in range(peers // chunk_peers):
        asked = [ask_ref[chunk * chunk_peers + i] for i in range(chunk_peers)]
        queries = jnp.concatenate([a[:per_peer] for a in asked], axis=0)
        tails = [a[per_peer:].astype(jnp.float32) for a in asked]
        spread = lambda i: jnp.concatenate(
            [jnp.broadcast_to(t[i : i + 1], (per_peer, width)) for t in tails], axis=0
        ).astype(jnp.bfloat16)
        exact_queries = jnp.concatenate([queries, spread(0)], axis=1)
        coarse_queries = jnp.concatenate([queries, spread(1)], axis=1)
        coarse = (
            lax.dot_general(
                coarse_queries, coarse_keys, contract_last, preferred_element_type=jnp.float32
            )
            * scale
            + log_page
        )
        tops, totals, outs = [], [], []
        for b in range(NEAR):
            scores = (
                lax.dot_general(
                    exact_queries, keys[b], contract_last, preferred_element_type=jnp.float32
                )
                * scale
            )
            mine = block_of == b
            top = jnp.maximum(
                jnp.max(scores, axis=1, keepdims=True),
                jnp.max(jnp.where(mine, coarse, FLOOR_SCORE), axis=1, keepdims=True),
            )
            top = jnp.maximum(top, FLOOR_SCORE)
            weights = jnp.exp(scores - top)
            coarse_weights = jnp.where(mine, jnp.exp(jnp.where(mine, coarse - top, 0.0)), 0.0)
            totals.append(
                jnp.sum(weights, axis=1, keepdims=True)
                + jnp.sum(coarse_weights, axis=1, keepdims=True)
            )
            outs.append(
                jnp.dot(
                    weights.astype(jnp.bfloat16),
                    page_refs[b][span : 2 * span, :],
                    preferred_element_type=jnp.float32,
                )
                + jnp.dot(
                    coarse_weights.astype(jnp.bfloat16),
                    coarse_values,
                    preferred_element_type=jnp.float32,
                )
            )
            tops.append(top)
        best = functools.reduce(jnp.maximum, tops)
        factors = [jnp.exp(t - best) for t in tops]
        total = sum(f * t for f, t in zip(factors, totals))
        out = sum(f * o for f, o in zip(factors, outs))
        stats = jnp.where(lane8 == 0, best, jnp.where(lane8 == 1, total, 0.0))
        stats = jnp.transpose(stats)[0:8]
        for i in range(chunk_peers):
            peer = chunk * chunk_peers + i
            reply_ref[peer, 0:per_peer, :] = out[i * per_peer : (i + 1) * per_peer]
            shift = (LANES - i * per_peer) % LANES
            reply_ref[peer, per_peer:, :] = pltpu.roll(stats, shift, 1) if shift else stats


def merge(heads, reply_ref, q_ref, nk_ref, nv_ref, o_ref):
    num_steps, _, num_heads, width = q_ref.shape
    group = num_heads // heads
    peers, height, _ = reply_ref.shape
    per_peer = height - 8
    scale = 1.0 / math.sqrt(width)
    stats = jnp.concatenate([reply_ref[p, per_peer:, :] for p in range(peers)], axis=0)
    stats = jnp.transpose(stats)[0:per_peer]
    step = lax.broadcasted_iota(jnp.int32, (per_peer, 1), 0) // group
    results = []
    for head in range(heads):
        queries = jnp.concatenate(
            [
                q_ref[s, 0, head * group : (head + 1) * group, :].astype(jnp.float32)
                for s in range(num_steps)
            ],
            axis=0,
        )
        scores = []
        for t in range(num_steps):
            key = nk_ref[t, 0, head : head + 1, :].astype(jnp.float32)
            scores.append(jnp.sum(queries * key, axis=1, keepdims=True) * scale)
        tail_top = functools.reduce(
            jnp.maximum, [jnp.where(step >= t, scores[t], FLOOR_SCORE) for t in range(num_steps)]
        )
        tail_total = jnp.zeros((per_peer, 1), jnp.float32)
        tail_out = jnp.zeros((per_peer, width), jnp.float32)
        for t in range(num_steps):
            weight = jnp.where(step >= t, jnp.exp(jnp.minimum(scores[t] - tail_top, 0.0)), 0.0)
            tail_total += weight
            value = nv_ref[t, 0, head : head + 1, :].astype(jnp.float32)
            tail_out += weight.astype(jnp.bfloat16).astype(jnp.float32) * value
        sources = range(head, peers, heads)
        tops = [stats[:, 8 * p : 8 * p + 1] for p in sources]
        totals = [stats[:, 8 * p + 1 : 8 * p + 2] for p in sources]
        best = functools.reduce(jnp.maximum, tops, tail_top)
        factor = jnp.exp(tail_top - best)
        numer, denom = factor * tail_out, factor * tail_total
        for p, top, total in zip(sources, tops, totals):
            factor = jnp.exp(top - best)
            numer += factor * reply_ref[p, 0:per_peer, :]
            denom += factor * total
        results.append(numer / denom)
    for s in range(num_steps):
        rows = [r[s * group : (s + 1) * group] for r in results]
        o_ref[s, 0] = jnp.concatenate(rows, axis=0).astype(o_ref.dtype)


VMEM = pl.BlockSpec(memory_space=pltpu.VMEM)
SMEM = pl.BlockSpec(memory_space=pltpu.SMEM)


def per_device(ring, queries, new_keys, step_new_values, keys, values, cent_keys, cent_values, slots, picks):
    num_steps, _, num_heads, width = queries.shape
    heads, span = keys.shape[:2]
    near = cent_keys.shape[1]
    peers = lax.axis_size("hi") * lax.axis_size("row")
    group = num_heads // heads
    height = num_steps * group + 8
    ask, pages = pl.pallas_call(
        functools.partial(prepare, heads, slots.shape[1]),
        out_shape=(
            jax.ShapeDtypeStruct((peers, height, width), jnp.bfloat16),
            jax.ShapeDtypeStruct((2 * span + 16, width), jnp.bfloat16),
        ),
        in_specs=[SMEM, SMEM] + [VMEM] * 5,
        out_specs=(VMEM, VMEM),
        name="prepare",
    )(picks, slots, queries, keys, values, cent_keys, cent_values)
    cores = lax.axis_size("row")
    every = [(z, c) for z in range(ring) for c in range(cores)]
    shift = lambda of: [(((z + of(c)) % ring) * cores + c, z * cores + c) for z, c in every]
    fetched = [pages] + [
        lax.ppermute(pages, RING + ("row",), shift(lambda c, i=i: near_offsets(c)[i]))
        for i in range(1, NEAR)
    ]
    asked = lax.all_to_all(ask, PEERS, 0, 0, tiled=True)
    flops = 4 * peers * (height - 8) * span * NEAR * width
    reply = pl.pallas_call(
        functools.partial(attend, span, near, ring),
        out_shape=jax.ShapeDtypeStruct((peers, height, width), jnp.float32),
        in_specs=[VMEM] * (1 + NEAR),
        out_specs=VMEM,
        cost_estimate=pl.CostEstimate(flops=flops, bytes_accessed=2**21, transcendentals=2**20),
        name="attend",
    )(asked, *fetched)
    reply = lax.all_to_all(reply, PEERS, 0, 0, tiled=True)
    return pl.pallas_call(
        functools.partial(merge, heads),
        out_shape=jax.ShapeDtypeStruct(queries.shape, jnp.bfloat16),
        in_specs=[VMEM] * 4,
        out_specs=VMEM,
        name="merge",
    )(reply, queries, new_keys, step_new_values)


def solution(mesh):
    sizes = mesh.shape
    names = [n for a in mesh.axis_names for n in (RING if a == "ctx" else (a,))]
    ring = sizes["ctx"]
    lengths = {**sizes, "hi": ring // NEAR, "lo": NEAR}
    split = jax.sharding.Mesh(mesh.devices.reshape([lengths[n] for n in names]), tuple(names))
    rows = ("groups",) + RING + ("row",)
    by_row = P(None, rows, "rep", None)
    by_page = P("rep", ("groups",) + RING, None)
    return jax.shard_map(
        functools.partial(per_device, ring),
        mesh=split,
        in_specs=(by_row,) * 3 + (by_page,) * 4 + (P("rep", "groups"), P(rows, "rep", None)),
        out_specs=by_row,
        check_vma=False,
    )
```

```python
import functools
import math

import jax
import jax.numpy as jnp
from jax import lax
from jax.experimental import pallas as pl
from jax.experimental.pallas import tpu as pltpu
from jax.sharding import PartitionSpec as P


FLOOR_SCORE = -10000.0
MASKED = -(2.0**100)
NEAR = 4
RING = ("hi", "lo")
PEERS = ("hi", "row")
LANES = 128


def place():
    return lax.axis_index("hi") * NEAR + lax.axis_index("lo"), lax.axis_index("row")


def near_offsets(core):
    return (0, 1, -1, 2 - 4 * core)


def pack_pages(k_ref, v_ref, ck_ref, cv_ref, pages_ref, ck_own, cv_own, arrived):
    core = lax.axis_index("row")
    span, width = k_ref.shape[1:]
    near = ck_ref.shape[1]
    copies = [
        pltpu.make_async_copy(source.at[core], target, arrived.at[i])
        for i, (source, target) in enumerate(
            (
                (k_ref, pages_ref.at[pl.ds(0, span)]),
                (v_ref, pages_ref.at[pl.ds(span, span)]),
                (ck_ref, ck_own),
                (cv_ref, cv_own),
            )
        )
    ]
    for copy in copies:
        copy.start()
    for copy in copies[::-1]:
        copy.wait()
    coarse = jnp.concatenate(
        [ck_own[...].astype(jnp.float32), cv_own[...].astype(jnp.float32)]
        + [jnp.zeros((16 - 2 * near, width), jnp.float32)],
        axis=0,
    )
    pages_ref[2 * span :, :] = coarse.astype(pages_ref.dtype)


def head_queries(q_ref, heads, head):
    num_steps, _, num_heads, _ = q_ref.shape
    group = num_heads // heads
    rows = slice(head * group, (head + 1) * group)
    return [q_ref[s, 0, rows, :].astype(jnp.float32) for s in range(num_steps)]


def pack_ask(heads, picks_ref, slots_ref, q_ref, ask_ref):
    width = q_ref.shape[3]
    lane = lax.broadcasted_iota(jnp.int32, (8, width), 1)
    sub = lax.broadcasted_iota(jnp.int32, (8, width), 0)
    for head in range(heads):
        slot_free = jnp.ones((8, width), jnp.float32)
        cluster_used = jnp.zeros((8, width), jnp.float32)
        for i in range(picks_ref.shape[2]):
            pick = picks_ref[0, head, i]
            slot_free = jnp.where(lane == slots_ref[head, pick], 0.0, slot_free)
            cluster_used = jnp.where(lane == pick, 1.0, cluster_used)
        masks = jnp.where(sub == 0, slot_free, jnp.where(sub == 1, cluster_used, 0.0))
        message = jnp.concatenate(head_queries(q_ref, heads, head) + [masks], axis=0)
        message = message.astype(ask_ref.dtype)
        for peer in range(head, ask_ref.shape[0], heads):
            ask_ref[peer] = message


def tail(heads, q_ref, nk_ref, nv_ref, out_ref, stat_ref):
    num_steps, _, num_heads, width = q_ref.shape
    per_peer = num_steps * num_heads // heads
    scale = 1.0 / math.sqrt(width)
    step = lax.broadcasted_iota(jnp.int32, (per_peer, 1), 0) // (num_heads // heads)
    lane = lax.broadcasted_iota(jnp.int32, (per_peer, width), 1)
    for head in range(heads):
        queries = jnp.concatenate(head_queries(q_ref, heads, head), axis=0)
        scores = []
        for t in range(num_steps):
            key = nk_ref[t, 0, head : head + 1, :].astype(jnp.float32)
            scores.append(jnp.sum(queries * key, axis=1, keepdims=True) * scale)
        top = functools.reduce(
            jnp.maximum, [jnp.where(step >= t, scores[t], FLOOR_SCORE) for t in range(num_steps)]
        )
        total = jnp.zeros((per_peer, 1), jnp.float32)
        out = jnp.zeros((per_peer, width), jnp.float32)
        for t in range(num_steps):
            weight = jnp.where(step >= t, jnp.exp(jnp.minimum(scores[t] - top, 0.0)), 0.0)
            total += weight
            value = nv_ref[t, 0, head : head + 1, :].astype(jnp.float32)
            out += weight.astype(jnp.bfloat16).astype(jnp.float32) * value
        out_ref[head] = out
        stat_ref[head] = jnp.where(lane == 0, top, total)


def attend(span, near, ring, ask_ref, *rest):
    page_refs, reply_ref = rest[:NEAR], rest[NEAR]
    peers, height, width = ask_ref.shape
    per_peer = height - 8
    scale = 1.0 / math.sqrt(width)
    log_page = math.log(span // near)
    chunk_peers = LANES // per_peer
    position, core = place()
    shards = [lax.rem(position + off + ring, ring) for off in near_offsets(core)]
    page = span // near
    lane = lax.broadcasted_iota(jnp.int32, (page, width), 1)
    keys = []
    for ref, shard in zip(page_refs, shards):
        picker = jnp.concatenate(
            [jnp.where(lane == shard * near + p, MASKED, 0.0) for p in range(near)], axis=0
        ).astype(jnp.bfloat16)
        keys.append(jnp.concatenate([ref[0:span, :], picker], axis=1))
    ends = [ref[2 * span :, :].astype(jnp.float32) for ref in page_refs]
    blank = jnp.zeros((LANES - near * NEAR, width), jnp.float32)
    coarse_keys = jnp.concatenate([e[0:near] for e in ends] + [blank], axis=0)
    coarse_values = jnp.concatenate([e[near : 2 * near] for e in ends] + [blank], axis=0)
    coarse_values = coarse_values.astype(jnp.bfloat16)
    row = lax.broadcasted_iota(jnp.int32, (LANES, width), 0)
    column = lax.broadcasted_iota(jnp.int32, (LANES, width), 1)
    cluster = jnp.full((LANES, width), -1, jnp.int32)
    for b, shard in enumerate(shards):
        cluster = jnp.where(row // near == b, shard * near + row - b * near, cluster)
    picker = jnp.where(column == cluster, MASKED, 0.0)
    coarse_keys = jnp.concatenate([coarse_keys, picker], axis=1).astype(jnp.bfloat16)
    block_of = lax.broadcasted_iota(jnp.int32, (LANES, LANES), 1) // near
    lane8 = lax.broadcasted_iota(jnp.int32, (LANES, LANES), 1)
    contract_last = (((1,), (1,)), ((), ()))

    for chunk in range(peers // chunk_peers):
        asked = [ask_ref[chunk * chunk_peers + i] for i in range(chunk_peers)]
        queries = jnp.concatenate([a[:per_peer] for a in asked], axis=0)
        tails = [a[per_peer:].astype(jnp.float32) for a in asked]
        spread = lambda i: jnp.concatenate(
            [jnp.broadcast_to(t[i : i + 1], (per_peer, width)) for t in tails], axis=0
        ).astype(jnp.bfloat16)
        exact_queries = jnp.concatenate([queries, spread(0)], axis=1)
        coarse_queries = jnp.concatenate([queries, spread(1)], axis=1)
        coarse = (
            lax.dot_general(
                coarse_queries, coarse_keys, contract_last, preferred_element_type=jnp.float32
            )
            * scale
            + log_page
        )
        tops, totals, outs = [], [], []
        for b in range(NEAR):
            scores = (
                lax.dot_general(
                    exact_queries, keys[b], contract_last, preferred_element_type=jnp.float32
                )
                * scale
            )
            mine = block_of == b
            top = jnp.maximum(
                jnp.max(scores, axis=1, keepdims=True),
                jnp.max(jnp.where(mine, coarse, FLOOR_SCORE), axis=1, keepdims=True),
            )
            top = jnp.maximum(top, FLOOR_SCORE)
            weights = jnp.exp(scores - top)
            coarse_weights = jnp.where(mine, jnp.exp(jnp.where(mine, coarse - top, 0.0)), 0.0)
            totals.append(
                jnp.sum(weights, axis=1, keepdims=True)
                + jnp.sum(coarse_weights, axis=1, keepdims=True)
            )
            outs.append(
                jnp.dot(
                    weights.astype(jnp.bfloat16),
                    page_refs[b][span : 2 * span, :],
                    preferred_element_type=jnp.float32,
                )
                + jnp.dot(
                    coarse_weights.astype(jnp.bfloat16),
                    coarse_values,
                    preferred_element_type=jnp.float32,
                )
            )
            tops.append(top)
        best = functools.reduce(jnp.maximum, tops)
        factors = [jnp.exp(t - best) for t in tops]
        total = sum(f * t for f, t in zip(factors, totals))
        out = sum(f * o for f, o in zip(factors, outs))
        stats = jnp.where(lane8 == 0, best, jnp.where(lane8 == 1, total, 0.0))
        stats = jnp.transpose(stats)[0:8]
        for i in range(chunk_peers):
            peer = chunk * chunk_peers + i
            reply_ref[peer, 0:per_peer, :] = out[i * per_peer : (i + 1) * per_peer]
            shift = (LANES - i * per_peer) % LANES
            reply_ref[peer, per_peer:, :] = pltpu.roll(stats, shift, 1) if shift else stats


def merge(heads, reply_ref, tail_ref, tail_stat_ref, o_ref):
    num_steps, _, num_heads, _ = o_ref.shape
    group = num_heads // heads
    peers, height, _ = reply_ref.shape
    per_peer = height - 8
    stats = jnp.concatenate([reply_ref[p, per_peer:, :] for p in range(peers)], axis=0)
    stats = jnp.transpose(stats)[0:per_peer]
    results = []
    for head in range(heads):
        sources = range(head, peers, heads)
        tops = [stats[:, 8 * p : 8 * p + 1] for p in sources]
        totals = [stats[:, 8 * p + 1 : 8 * p + 2] for p in sources]
        tail_top = tail_stat_ref[head, :, 0:1]
        best = functools.reduce(jnp.maximum, tops, tail_top)
        factor = jnp.exp(tail_top - best)
        numer, denom = factor * tail_ref[head], factor * tail_stat_ref[head, :, 1:2]
        for p, top, total in zip(sources, tops, totals):
            factor = jnp.exp(top - best)
            numer += factor * reply_ref[p, 0:per_peer, :]
            denom += factor * total
        results.append(numer / denom)
    for s in range(num_steps):
        rows = [r[s * group : (s + 1) * group] for r in results]
        o_ref[s, 0] = jnp.concatenate(rows, axis=0).astype(o_ref.dtype)


VMEM = pl.BlockSpec(memory_space=pltpu.VMEM)
SMEM = pl.BlockSpec(memory_space=pltpu.SMEM)


def on_core(kernel, out_shape, in_specs, flops, mib, scratch=()):
    many = isinstance(out_shape, tuple)
    return pl.pallas_call(
        kernel,
        out_shape=out_shape,
        in_specs=in_specs,
        out_specs=(VMEM,) * len(out_shape) if many else VMEM,
        scratch_shapes=scratch,
        cost_estimate=pl.CostEstimate(flops=flops, bytes_accessed=2**20, transcendentals=0),
        compiler_params=pltpu.CompilerParams(vmem_limit_bytes=mib * 2**20),
    )


def per_device(ring, queries, new_keys, step_new_values, keys, values, cent_keys, cent_values, slots, picks):
    num_steps, _, num_heads, width = queries.shape
    heads, span = keys.shape[:2]
    near = cent_keys.shape[1]
    cores = lax.axis_size("row")
    peers = lax.axis_size("hi") * cores
    per_peer = num_steps * num_heads // heads
    height = per_peer + 8
    shape = jax.ShapeDtypeStruct
    pages = on_core(
        pack_pages,
        shape((2 * span + 16, width), jnp.bfloat16),
        [pl.BlockSpec(memory_space=pl.ANY)] * 4,
        2**16,
        4,
        [pltpu.VMEM((near, width), jnp.bfloat16)] * 2 + [pltpu.SemaphoreType.DMA((4,))],
    )(keys, values, cent_keys, cent_values)
    every = [(z, c) for z in range(ring) for c in range(cores)]
    shift = lambda of: [(((z + of(c)) % ring) * cores + c, z * cores + c) for z, c in every]
    fetched = [pages]
    for i in range(1, NEAR):
        pairs = shift(lambda c: near_offsets(c)[i])
        fetched.append(lax.ppermute(pages, RING + ("row",), pairs))
    ask = on_core(
        functools.partial(pack_ask, heads),
        shape((peers, height, width), jnp.bfloat16),
        [SMEM, SMEM, VMEM],
        2**16,
        4,
    )(picks, slots, queries)
    asked = lax.all_to_all(ask, PEERS, 0, 0, tiled=True)
    tail_out, tail_stat = on_core(
        functools.partial(tail, heads),
        (shape((heads, per_peer, width), jnp.float32),) * 2,
        [VMEM] * 3,
        2**22,
        4,
    )(queries, new_keys, step_new_values)
    reply = on_core(
        functools.partial(attend, span, near, ring),
        shape((peers, height, width), jnp.float32),
        [VMEM] * (1 + NEAR),
        4 * peers * per_peer * span * NEAR * width,
        20,
    )(asked, *fetched)
    reply = lax.all_to_all(reply, PEERS, 0, 0, tiled=True)
    return on_core(
        functools.partial(merge, heads), shape(queries.shape, jnp.bfloat16), [VMEM] * 3, 2**20, 8
    )(reply, tail_out, tail_stat)


def solution(mesh):
    sizes = mesh.shape
    names = [n for a in mesh.axis_names for n in (RING if a == "ctx" else (a,))]
    ring = sizes["ctx"]
    lengths = {**sizes, "hi": ring // NEAR, "lo": NEAR}
    split = jax.sharding.Mesh(mesh.devices.reshape([lengths[n] for n in names]), tuple(names))
    rows = ("groups",) + RING + ("row",)
    by_row = P(None, rows, "rep", None)
    by_page = P("rep", ("groups",) + RING, None)
    return jax.shard_map(
        functools.partial(per_device, ring),
        mesh=split,
        in_specs=(by_row,) * 3 + (by_page,) * 4 + (P("rep", "groups"), P(rows, "rep", None)),
        out_specs=by_row,
        check_vma=False,
    )
```

```python
import functools
import math

import jax
import jax.numpy as jnp
from jax import lax
from jax.experimental import pallas as pl
from jax.experimental.pallas import tpu as pltpu
from jax.sharding import PartitionSpec as P


FLOOR_SCORE = -10000.0
MASKED = -(2.0**100)
NEAR = 4
RING = ("hi", "lo")
PEERS = ("hi", "row")
LANES = 128
SMALLEST = 2.0**-100
LOW_SCALE = 1024.0


def as_bf16(x):
    return x.astype(jnp.bfloat16).astype(jnp.float32)


def place():
    return lax.axis_index("hi") * NEAR + lax.axis_index("lo"), lax.axis_index("row")


def near_offsets(core):
    return (0, 1, -1, 2 - 4 * core)


def head_queries(q_ref, heads, head):
    num_steps, _, num_heads, _ = q_ref.shape
    group = num_heads // heads
    rows = slice(head * group, (head + 1) * group)
    return [q_ref[s, 0, rows, :].astype(jnp.float32) for s in range(num_steps)]


def prepare(
    heads, picks_ref, slots_ref, q_hbm, k_ref, v_ref, ck_ref, cv_ref, pages_ref, ask_ref,
    q_ref, ck_own, cv_own, arrived,
):
    core = lax.axis_index("row")
    span, width = k_ref.shape[1:]
    near = ck_ref.shape[1]
    moves = (
        (q_hbm, q_ref),
        (ck_ref.at[core], ck_own),
        (cv_ref.at[core], cv_own),
        (k_ref.at[core], pages_ref.at[pl.ds(0, span)]),
        (v_ref.at[core], pages_ref.at[pl.ds(span, span)]),
    )
    copies = [pltpu.make_async_copy(*move, arrived.at[i]) for i, move in enumerate(moves)]
    for copy in copies:
        copy.start()
    lane = lax.broadcasted_iota(jnp.int32, (8, width), 1)
    sub = lax.broadcasted_iota(jnp.int32, (8, width), 0)
    masks = []
    for head in range(heads):
        slot_free = jnp.ones((8, width), jnp.float32)
        cluster_used = jnp.zeros((8, width), jnp.float32)
        for i in range(picks_ref.shape[2]):
            pick = picks_ref[0, head, i]
            slot_free = jnp.where(lane == slots_ref[head, pick], 0.0, slot_free)
            cluster_used = jnp.where(lane == pick, 1.0, cluster_used)
        masks.append(jnp.where(sub == 0, slot_free, jnp.where(sub == 1, cluster_used, 0.0)))
    copies[0].wait()
    for head in range(heads):
        message = jnp.concatenate(head_queries(q_ref, heads, head) + [masks[head]], axis=0)
        message = message.astype(ask_ref.dtype)
        for peer in range(head, ask_ref.shape[0], heads):
            ask_ref[peer] = message
    for copy in copies[1:3]:
        copy.wait()
    coarse = jnp.concatenate(
        [ck_own[...].astype(jnp.float32), cv_own[...].astype(jnp.float32)]
        + [jnp.zeros((16 - 2 * near, width), jnp.float32)],
        axis=0,
    )
    pages_ref[2 * span :, :] = coarse.astype(pages_ref.dtype)
    for copy in copies[3:]:
        copy.wait()


def tail(heads, q_ref, nk_ref, nv_ref, out_ref, stat_ref):
    num_steps, _, num_heads, width = q_ref.shape
    per_peer = num_steps * num_heads // heads
    scale = 1.0 / math.sqrt(width)
    step = lax.broadcasted_iota(jnp.int32, (per_peer, 1), 0) // (num_heads // heads)
    lane = lax.broadcasted_iota(jnp.int32, (per_peer, width), 1)
    for head in range(heads):
        queries = jnp.concatenate(head_queries(q_ref, heads, head), axis=0)
        scores = []
        for t in range(num_steps):
            key = nk_ref[t, 0, head : head + 1, :].astype(jnp.float32)
            scores.append(jnp.sum(queries * key, axis=1, keepdims=True) * scale)
        top = functools.reduce(
            jnp.maximum, [jnp.where(step >= t, scores[t], FLOOR_SCORE) for t in range(num_steps)]
        )
        total = jnp.zeros((per_peer, 1), jnp.float32)
        out = jnp.zeros((per_peer, width), jnp.float32)
        for t in range(num_steps):
            weight = jnp.where(step >= t, jnp.exp(jnp.minimum(scores[t] - top, 0.0)), 0.0)
            total += weight
            value = nv_ref[t, 0, head : head + 1, :].astype(jnp.float32)
            out += weight.astype(jnp.bfloat16).astype(jnp.float32) * value
        out_ref[head] = out
        stat_ref[head] = jnp.where(lane == 0, top, total)


def attend(span, near, ring, ask_ref, *rest):
    page_refs, reply_ref = rest[:NEAR], rest[NEAR]
    peers, height, width = ask_ref.shape
    per_peer = height - 8
    scale = 1.0 / math.sqrt(width)
    log_page = math.log(span // near)
    chunk_peers = LANES // per_peer
    position, core = place()
    shards = [lax.rem(position + off + ring, ring) for off in near_offsets(core)]
    page = span // near
    lane = lax.broadcasted_iota(jnp.int32, (page, width), 1)
    keys = []
    for ref, shard in zip(page_refs, shards):
        picker = jnp.concatenate(
            [jnp.where(lane == shard * near + p, MASKED, 0.0) for p in range(near)], axis=0
        ).astype(jnp.bfloat16)
        keys.append(jnp.concatenate([ref[0:span, :], picker], axis=1))
    ends = [ref[2 * span :, :].astype(jnp.float32) for ref in page_refs]
    blank = jnp.zeros((LANES - near * NEAR, width), jnp.float32)
    coarse_keys = jnp.concatenate([e[0:near] for e in ends] + [blank], axis=0)
    coarse_values = jnp.concatenate([e[near : 2 * near] for e in ends] + [blank], axis=0)
    coarse_values = coarse_values.astype(jnp.bfloat16)
    row = lax.broadcasted_iota(jnp.int32, (LANES, width), 0)
    column = lax.broadcasted_iota(jnp.int32, (LANES, width), 1)
    cluster = jnp.full((LANES, width), -1, jnp.int32)
    for b, shard in enumerate(shards):
        cluster = jnp.where(row // near == b, shard * near + row - b * near, cluster)
    picker = jnp.where(column == cluster, MASKED, 0.0)
    coarse_keys = jnp.concatenate([coarse_keys, picker], axis=1).astype(jnp.bfloat16)
    block_of = lax.broadcasted_iota(jnp.int32, (LANES, LANES), 1) // near
    lane8 = lax.broadcasted_iota(jnp.int32, (LANES, LANES), 1)
    contract_last = (((1,), (1,)), ((), ()))

    for chunk in range(peers // chunk_peers):
        asked = [ask_ref[chunk * chunk_peers + i] for i in range(chunk_peers)]
        queries = jnp.concatenate([a[:per_peer] for a in asked], axis=0)
        tails = [a[per_peer:].astype(jnp.float32) for a in asked]
        spread = lambda i: jnp.concatenate(
            [jnp.broadcast_to(t[i : i + 1], (per_peer, width)) for t in tails], axis=0
        ).astype(jnp.bfloat16)
        exact_queries = jnp.concatenate([queries, spread(0)], axis=1)
        coarse_queries = jnp.concatenate([queries, spread(1)], axis=1)
        coarse = (
            lax.dot_general(
                coarse_queries, coarse_keys, contract_last, preferred_element_type=jnp.float32
            )
            * scale
            + log_page
        )
        tops, totals, outs = [], [], []
        for b in range(NEAR):
            scores = (
                lax.dot_general(
                    exact_queries, keys[b], contract_last, preferred_element_type=jnp.float32
                )
                * scale
            )
            mine = block_of == b
            top = jnp.maximum(
                jnp.max(scores, axis=1, keepdims=True),
                jnp.max(jnp.where(mine, coarse, FLOOR_SCORE), axis=1, keepdims=True),
            )
            top = jnp.maximum(top, FLOOR_SCORE)
            weights = jnp.exp(scores - top)
            coarse_weights = jnp.where(mine, jnp.exp(jnp.where(mine, coarse - top, 0.0)), 0.0)
            totals.append(
                jnp.sum(weights, axis=1, keepdims=True)
                + jnp.sum(coarse_weights, axis=1, keepdims=True)
            )
            outs.append(
                jnp.dot(
                    weights.astype(jnp.bfloat16),
                    page_refs[b][span : 2 * span, :],
                    preferred_element_type=jnp.float32,
                )
                + jnp.dot(
                    coarse_weights.astype(jnp.bfloat16),
                    coarse_values,
                    preferred_element_type=jnp.float32,
                )
            )
            tops.append(top)
        best = functools.reduce(jnp.maximum, tops)
        factors = [jnp.exp(t - best) for t in tops]
        total = sum(f * t for f, t in zip(factors, totals))
        out = sum(f * o for f, o in zip(factors, outs))
        level = jnp.where(total > 0.0, best + jnp.log(total), 2 * FLOOR_SCORE)
        out = out * jnp.where(total > 0.0, 1.0 / total, 0.0)
        largest = jnp.max(jnp.abs(out), axis=1, keepdims=True)
        power = jnp.ceil(jnp.log2(jnp.maximum(largest, SMALLEST)))
        out = out * jnp.exp2(-power)
        high = as_bf16(level)
        middle = as_bf16(level - high)
        low = (level - high - middle) * LOW_SCALE
        stats = jnp.zeros((LANES, LANES), jnp.float32)
        for i, part in enumerate((high, middle, low, power)):
            stats = jnp.where(lane8 == i, part, stats)
        stats = jnp.transpose(stats)[0:8]
        turns = [pltpu.roll(stats, i * per_peer, 1) if i else stats for i in range(chunk_peers)]
        part_of = lax.broadcasted_iota(jnp.int32, (8, LANES), 1) // per_peer
        first_row = lax.broadcasted_iota(jnp.int32, (8, LANES), 0) == 0
        for i in range(chunk_peers):
            peer = chunk * chunk_peers + i
            reply_ref[peer, 0:per_peer, :] = out[i * per_peer : (i + 1) * per_peer]
            line = jnp.zeros((8, LANES), jnp.float32)
            for part in range(chunk_peers):
                turned = turns[(part - i) % chunk_peers][part : part + 1]
                line = jnp.where((part_of == part) & first_row, turned, line)
            reply_ref[peer, per_peer:, :] = line


def merge(heads, reply_ref, tail_ref, tail_stat_ref, o_ref):
    num_steps, _, num_heads, _ = o_ref.shape
    group = num_heads // heads
    peers, height, _ = reply_ref.shape
    per_peer = height - 8
    stats = [reply_ref[p, per_peer : per_peer + 1, :] for p in range(peers)]
    stats = jnp.transpose(
        jnp.concatenate(stats + [jnp.zeros((LANES - peers, LANES), jnp.float32)], axis=0)
    )
    high, middle, low, power = (stats[i * per_peer : (i + 1) * per_peer] for i in range(4))
    levels = high + (middle + low * (1.0 / LOW_SCALE))
    powers = jnp.exp2(power)
    results = []
    for head in range(heads):
        sources = range(head, peers, heads)
        tops = [levels[:, p : p + 1] for p in sources]
        tail_top = tail_stat_ref[head, :, 0:1]
        best = functools.reduce(jnp.maximum, tops, tail_top)
        factor = jnp.exp(tail_top - best)
        numer, denom = factor * tail_ref[head], factor * tail_stat_ref[head, :, 1:2]
        for p, top in zip(sources, tops):
            factor = jnp.exp(top - best)
            numer += (factor * powers[:, p : p + 1]) * reply_ref[p, 0:per_peer, :]
            denom += factor
        results.append(numer / denom)
    for s in range(num_steps):
        rows = [r[s * group : (s + 1) * group] for r in results]
        o_ref[s, 0] = jnp.concatenate(rows, axis=0).astype(o_ref.dtype)


VMEM = pl.BlockSpec(memory_space=pltpu.VMEM)
SMEM = pl.BlockSpec(memory_space=pltpu.SMEM)
HBM = pl.BlockSpec(memory_space=pltpu.HBM)


def on_core(kernel, out_shape, in_specs, flops, mib, scratch=()):
    many = isinstance(out_shape, tuple)
    return pl.pallas_call(
        kernel,
        out_shape=out_shape,
        in_specs=in_specs,
        out_specs=(VMEM,) * len(out_shape) if many else VMEM,
        scratch_shapes=scratch,
        cost_estimate=pl.CostEstimate(flops=flops, bytes_accessed=2**20, transcendentals=0),
        compiler_params=pltpu.CompilerParams(vmem_limit_bytes=mib * 2**20),
    )


def per_device(ring, queries, new_keys, step_new_values, keys, values, cent_keys, cent_values, slots, picks):
    num_steps, _, num_heads, width = queries.shape
    heads, span = keys.shape[:2]
    near = cent_keys.shape[1]
    cores = lax.axis_size("row")
    peers = lax.axis_size("hi") * cores
    per_peer = num_steps * num_heads // heads
    height = per_peer + 8
    shape = jax.ShapeDtypeStruct
    pages, ask = on_core(
        functools.partial(prepare, heads),
        (
            shape((2 * span + 16, width), jnp.bfloat16),
            shape((peers, height, width), jnp.bfloat16),
        ),
        [SMEM] * 2 + [HBM] * 5,
        2**16,
        60,
        [pltpu.VMEM(queries.shape, jnp.bfloat16)]
        + [pltpu.VMEM((near, width), jnp.bfloat16)] * 2
        + [pltpu.SemaphoreType.DMA((5,))],
    )(picks, slots, queries, keys, values, cent_keys, cent_values)
    every = [(z, c) for z in range(ring) for c in range(cores)]
    shift = lambda of: [(((z + of(c)) % ring) * cores + c, z * cores + c) for z, c in every]
    fetched = [pages]
    for i in range(1, NEAR):
        pairs = shift(lambda c: near_offsets(c)[i])
        fetched.append(lax.ppermute(pages, RING + ("row",), pairs))
    asked = lax.all_to_all(ask, PEERS, 0, 0, tiled=True)
    tail_out, tail_stat = on_core(
        functools.partial(tail, heads),
        (shape((heads, per_peer, width), jnp.float32),) * 2,
        [VMEM] * 3,
        2**22,
        4,
    )(queries, new_keys, step_new_values)
    reply = on_core(
        functools.partial(attend, span, near, ring),
        shape((peers, height, width), jnp.float32),
        [VMEM] * (1 + NEAR),
        4 * peers * per_peer * span * NEAR * width,
        20,
    )(asked, *fetched)
    reply = lax.all_to_all(reply.astype(jnp.float16), PEERS, 0, 0, tiled=True)
    reply = reply.astype(jnp.float32)
    return on_core(
        functools.partial(merge, heads), shape(queries.shape, jnp.bfloat16), [VMEM] * 3, 2**20, 8
    )(reply, tail_out, tail_stat)


def solution(mesh):
    sizes = mesh.shape
    names = [n for a in mesh.axis_names for n in (RING if a == "ctx" else (a,))]
    ring = sizes["ctx"]
    lengths = {**sizes, "hi": ring // NEAR, "lo": NEAR}
    split = jax.sharding.Mesh(mesh.devices.reshape([lengths[n] for n in names]), tuple(names))
    rows = ("groups",) + RING + ("row",)
    by_row = P(None, rows, "rep", None)
    by_page = P("rep", ("groups",) + RING, None)
    return jax.shard_map(
        functools.partial(per_device, ring),
        mesh=split,
        in_specs=(by_row,) * 3 + (by_page,) * 4 + (P("rep", "groups"), P(rows, "rep", None)),
        out_specs=by_row,
        check_vma=False,
    )
```

```python
import functools
import math

import jax
import jax.numpy as jnp
from jax import lax
from jax.experimental import pallas as pl
from jax.experimental.pallas import tpu as pltpu
from jax.sharding import PartitionSpec as P


FLOOR_SCORE = -10000.0
MASKED = -(2.0**100)
NEAR = 4
RING = ("hi", "lo")
PEERS = ("hi", "row")
LANES = 128
EXTRA = 2
SMALLEST = 2.0**-100
LOW_SCALE = 1024.0


def as_bf16(x):
    return x.astype(jnp.bfloat16).astype(jnp.float32)


def place():
    return lax.axis_index("hi") * NEAR + lax.axis_index("lo"), lax.axis_index("row")


def near_offsets(core):
    return (0, 1, -1, 2 - 4 * core)


def head_queries(q_ref, heads, head):
    num_steps, _, num_heads, _ = q_ref.shape
    group = num_heads // heads
    rows = slice(head * group, (head + 1) * group)
    return [q_ref[s, 0, rows, :].astype(jnp.float32) for s in range(num_steps)]


def prepare(
    heads, picks_ref, slots_ref, q_hbm, k_ref, v_ref, ck_ref, cv_ref, pages_ref, ask_ref,
    q_ref, ck_own, cv_own, arrived,
):
    core = lax.axis_index("row")
    span, width = k_ref.shape[1:]
    near = ck_ref.shape[1]
    moves = (
        (q_hbm, q_ref),
        (ck_ref.at[core], ck_own),
        (cv_ref.at[core], cv_own),
        (k_ref.at[core], pages_ref.at[pl.ds(0, span)]),
        (v_ref.at[core], pages_ref.at[pl.ds(span, span)]),
    )
    copies = [pltpu.make_async_copy(*move, arrived.at[i]) for i, move in enumerate(moves)]
    for copy in copies:
        copy.start()
    lane = lax.broadcasted_iota(jnp.int32, (8, width), 1)
    sub = lax.broadcasted_iota(jnp.int32, (8, width), 0)
    masks = []
    for head in range(heads):
        slot_free = jnp.ones((8, width), jnp.float32)
        cluster_used = jnp.zeros((8, width), jnp.float32)
        for i in range(picks_ref.shape[2]):
            pick = picks_ref[0, head, i]
            slot_free = jnp.where(lane == slots_ref[head, pick], 0.0, slot_free)
            cluster_used = jnp.where(lane == pick, 1.0, cluster_used)
        masks.append(jnp.where(sub == 0, slot_free, jnp.where(sub == 1, cluster_used, 0.0)))
    copies[0].wait()
    for head in range(heads):
        message = jnp.concatenate(head_queries(q_ref, heads, head) + [masks[head]], axis=0)
        height = message.shape[0] - 8 + EXTRA
        message = message[0:height].astype(ask_ref.dtype)
        for peer in range(head, ask_ref.shape[0] // height, heads):
            ask_ref[peer * height : (peer + 1) * height, :] = message
    for copy in copies[1:3]:
        copy.wait()
    coarse = jnp.concatenate(
        [ck_own[...].astype(jnp.float32), cv_own[...].astype(jnp.float32)]
        + [jnp.zeros((16 - 2 * near, width), jnp.float32)],
        axis=0,
    )
    pages_ref[2 * span :, :] = coarse.astype(pages_ref.dtype)
    for copy in copies[3:]:
        copy.wait()


def tail(heads, q_ref, nk_ref, nv_ref, out_ref, stat_ref):
    num_steps, _, num_heads, width = q_ref.shape
    per_peer = num_steps * num_heads // heads
    scale = 1.0 / math.sqrt(width)
    step = lax.broadcasted_iota(jnp.int32, (per_peer, 1), 0) // (num_heads // heads)
    lane = lax.broadcasted_iota(jnp.int32, (per_peer, width), 1)
    for head in range(heads):
        queries = jnp.concatenate(head_queries(q_ref, heads, head), axis=0)
        scores = []
        for t in range(num_steps):
            key = nk_ref[t, 0, head : head + 1, :].astype(jnp.float32)
            scores.append(jnp.sum(queries * key, axis=1, keepdims=True) * scale)
        top = functools.reduce(
            jnp.maximum, [jnp.where(step >= t, scores[t], FLOOR_SCORE) for t in range(num_steps)]
        )
        total = jnp.zeros((per_peer, 1), jnp.float32)
        out = jnp.zeros((per_peer, width), jnp.float32)
        for t in range(num_steps):
            weight = jnp.where(step >= t, jnp.exp(jnp.minimum(scores[t] - top, 0.0)), 0.0)
            total += weight
            value = nv_ref[t, 0, head : head + 1, :].astype(jnp.float32)
            out += weight.astype(jnp.bfloat16).astype(jnp.float32) * value
        out_ref[head] = out
        stat_ref[head] = jnp.where(lane == 0, top, total)


def attend(span, near, ring, peers, ask_ref, *rest):
    page_refs, reply_ref = rest[:NEAR], rest[NEAR]
    width = ask_ref.shape[1]
    height = ask_ref.shape[0] // peers
    per_peer = height - EXTRA
    scale = 1.0 / math.sqrt(width)
    log_page = math.log(span // near)
    chunk_peers = LANES // per_peer
    position, core = place()
    shards = [lax.rem(position + off + ring, ring) for off in near_offsets(core)]
    page = span // near
    lane = lax.broadcasted_iota(jnp.int32, (page, width), 1)
    keys = []
    for ref, shard in zip(page_refs, shards):
        picker = jnp.concatenate(
            [jnp.where(lane == shard * near + p, MASKED, 0.0) for p in range(near)], axis=0
        ).astype(jnp.bfloat16)
        keys.append(jnp.concatenate([ref[0:span, :], picker], axis=1))
    ends = [ref[2 * span :, :].astype(jnp.float32) for ref in page_refs]
    blank = jnp.zeros((LANES - near * NEAR, width), jnp.float32)
    coarse_keys = jnp.concatenate([e[0:near] for e in ends] + [blank], axis=0)
    coarse_values = jnp.concatenate([e[near : 2 * near] for e in ends] + [blank], axis=0)
    coarse_values = coarse_values.astype(jnp.bfloat16)
    row = lax.broadcasted_iota(jnp.int32, (LANES, width), 0)
    column = lax.broadcasted_iota(jnp.int32, (LANES, width), 1)
    cluster = jnp.full((LANES, width), -1, jnp.int32)
    for b, shard in enumerate(shards):
        cluster = jnp.where(row // near == b, shard * near + row - b * near, cluster)
    picker = jnp.where(column == cluster, MASKED, 0.0)
    coarse_keys = jnp.concatenate([coarse_keys, picker], axis=1).astype(jnp.bfloat16)
    block_of = lax.broadcasted_iota(jnp.int32, (LANES, LANES), 1) // near
    lane8 = lax.broadcasted_iota(jnp.int32, (LANES, LANES), 1)
    contract_last = (((1,), (1,)), ((), ()))

    for chunk in range(peers // chunk_peers):
        first = chunk * chunk_peers * height
        asked = ask_ref[first : first + chunk_peers * height, :].astype(jnp.float32)
        asked = [asked[i * height : (i + 1) * height] for i in range(chunk_peers)]
        queries = jnp.concatenate([a[:per_peer] for a in asked], axis=0).astype(jnp.bfloat16)
        tails = [a[per_peer:] for a in asked]
        spread = lambda i: jnp.concatenate(
            [jnp.broadcast_to(t[i : i + 1], (per_peer, width)) for t in tails], axis=0
        ).astype(jnp.bfloat16)
        exact_queries = jnp.concatenate([queries, spread(0)], axis=1)
        coarse_queries = jnp.concatenate([queries, spread(1)], axis=1)
        coarse = (
            lax.dot_general(
                coarse_queries, coarse_keys, contract_last, preferred_element_type=jnp.float32
            )
            * scale
            + log_page
        )
        tops, totals, outs = [], [], []
        for b in range(NEAR):
            scores = (
                lax.dot_general(
                    exact_queries, keys[b], contract_last, preferred_element_type=jnp.float32
                )
                * scale
            )
            mine = block_of == b
            top = jnp.maximum(
                jnp.max(scores, axis=1, keepdims=True),
                jnp.max(jnp.where(mine, coarse, FLOOR_SCORE), axis=1, keepdims=True),
            )
            top = jnp.maximum(top, FLOOR_SCORE)
            weights = jnp.exp(scores - top)
            coarse_weights = jnp.where(mine, jnp.exp(jnp.where(mine, coarse - top, 0.0)), 0.0)
            totals.append(
                jnp.sum(weights, axis=1, keepdims=True)
                + jnp.sum(coarse_weights, axis=1, keepdims=True)
            )
            outs.append(
                jnp.dot(
                    weights.astype(jnp.bfloat16),
                    page_refs[b][span : 2 * span, :],
                    preferred_element_type=jnp.float32,
                )
                + jnp.dot(
                    coarse_weights.astype(jnp.bfloat16),
                    coarse_values,
                    preferred_element_type=jnp.float32,
                )
            )
            tops.append(top)
        best = functools.reduce(jnp.maximum, tops)
        factors = [jnp.exp(t - best) for t in tops]
        total = sum(f * t for f, t in zip(factors, totals))
        out = sum(f * o for f, o in zip(factors, outs))
        level = jnp.where(total > 0.0, best + jnp.log(total), 2 * FLOOR_SCORE)
        out = out * jnp.where(total > 0.0, 1.0 / total, 0.0)
        largest = jnp.max(jnp.abs(out), axis=1, keepdims=True)
        power = jnp.ceil(jnp.log2(jnp.maximum(largest, SMALLEST)))
        out = out * jnp.exp2(-power)
        high = as_bf16(level)
        middle = as_bf16(level - high)
        low = (level - high - middle) * LOW_SCALE
        stats = jnp.zeros((LANES, LANES), jnp.float32)
        for i, part in enumerate((high, middle, low, power)):
            stats = jnp.where(lane8 == i, part, stats)
        stats = jnp.transpose(stats)[0:8]
        turns = [pltpu.roll(stats, i * per_peer, 1) if i else stats for i in range(chunk_peers)]
        part_of = lax.broadcasted_iota(jnp.int32, (EXTRA, LANES), 1) // per_peer
        for i in range(chunk_peers):
            at = first + i * height
            reply_ref[at : at + per_peer, :] = out[i * per_peer : (i + 1) * per_peer]
            line = jnp.zeros((EXTRA, LANES), jnp.float32)
            for part in range(chunk_peers):
                turned = turns[(part - i) % chunk_peers][part : part + 1]
                line = jnp.where(part_of == part, turned, line)
            reply_ref[at + per_peer : at + height, :] = line


def merge(heads, peers, reply_ref, tail_ref, tail_stat_ref, o_ref):
    num_steps, _, num_heads, _ = o_ref.shape
    group = num_heads // heads
    height = reply_ref.shape[0] // peers
    per_peer = height - EXTRA
    replies = [reply_ref[p * height : (p + 1) * height, :] for p in range(peers)]
    stats = [r[per_peer : per_peer + 1] for r in replies]
    stats = jnp.transpose(
        jnp.concatenate(stats + [jnp.zeros((LANES - peers, LANES), jnp.float32)], axis=0)
    )
    high, middle, low, power = (stats[i * per_peer : (i + 1) * per_peer] for i in range(4))
    levels = high + (middle + low * (1.0 / LOW_SCALE))
    powers = jnp.exp2(power)
    results = []
    for head in range(heads):
        sources = range(head, peers, heads)
        tops = [levels[:, p : p + 1] for p in sources]
        tail_top = tail_stat_ref[head, :, 0:1]
        best = functools.reduce(jnp.maximum, tops, tail_top)
        factor = jnp.exp(tail_top - best)
        numer, denom = factor * tail_ref[head], factor * tail_stat_ref[head, :, 1:2]
        for p, top in zip(sources, tops):
            factor = jnp.exp(top - best)
            numer += (factor * powers[:, p : p + 1]) * replies[p][0:per_peer]
            denom += factor
        results.append(numer / denom)
    for s in range(num_steps):
        rows = [r[s * group : (s + 1) * group] for r in results]
        o_ref[s, 0] = jnp.concatenate(rows, axis=0).astype(o_ref.dtype)


VMEM = pl.BlockSpec(memory_space=pltpu.VMEM)
SMEM = pl.BlockSpec(memory_space=pltpu.SMEM)
HBM = pl.BlockSpec(memory_space=pltpu.HBM)


def on_core(kernel, out_shape, in_specs, flops, mib, scratch=()):
    many = isinstance(out_shape, tuple)
    return pl.pallas_call(
        kernel,
        out_shape=out_shape,
        in_specs=in_specs,
        out_specs=(VMEM,) * len(out_shape) if many else VMEM,
        scratch_shapes=scratch,
        cost_estimate=pl.CostEstimate(flops=flops, bytes_accessed=2**20, transcendentals=0),
        compiler_params=pltpu.CompilerParams(vmem_limit_bytes=mib * 2**20),
    )


def exchange(messages, peers):
    pairs = messages.reshape(peers, -1, 2, messages.shape[1])
    return lax.all_to_all(pairs, PEERS, 0, 0, tiled=True).reshape(messages.shape)


def per_device(ring, queries, new_keys, step_new_values, keys, values, cent_keys, cent_values, slots, picks):
    num_steps, _, num_heads, width = queries.shape
    heads, span = keys.shape[:2]
    near = cent_keys.shape[1]
    cores = lax.axis_size("row")
    peers = lax.axis_size("hi") * cores
    per_peer = num_steps * num_heads // heads
    height = per_peer + EXTRA
    shape = jax.ShapeDtypeStruct
    pages, ask = on_core(
        functools.partial(prepare, heads),
        (
            shape((2 * span + 16, width), jnp.bfloat16),
            shape((peers * height, width), jnp.bfloat16),
        ),
        [SMEM] * 2 + [HBM] * 5,
        2**16,
        60,
        [pltpu.VMEM(queries.shape, jnp.bfloat16)]
        + [pltpu.VMEM((near, width), jnp.bfloat16)] * 2
        + [pltpu.SemaphoreType.DMA((5,))],
    )(picks, slots, queries, keys, values, cent_keys, cent_values)
    every = [(z, c) for z in range(ring) for c in range(cores)]
    shift = lambda of: [(((z + of(c)) % ring) * cores + c, z * cores + c) for z, c in every]
    fetched = [pages]
    for i in range(1, NEAR):
        pairs = shift(lambda c: near_offsets(c)[i])
        fetched.append(lax.ppermute(pages, RING + ("row",), pairs))
    asked = exchange(ask, peers)
    tail_out, tail_stat = on_core(
        functools.partial(tail, heads),
        (shape((heads, per_peer, width), jnp.float32),) * 2,
        [VMEM] * 3,
        2**22,
        4,
    )(queries, new_keys, step_new_values)
    reply = on_core(
        functools.partial(attend, span, near, ring, peers),
        shape((peers * height, width), jnp.float32),
        [VMEM] * (1 + NEAR),
        4 * peers * per_peer * span * NEAR * width,
        20,
    )(asked, *fetched)
    reply = exchange(reply.astype(jnp.float16), peers).astype(jnp.float32)
    return on_core(
        functools.partial(merge, heads, peers),
        shape(queries.shape, jnp.bfloat16),
        [VMEM] * 3,
        2**20,
        8,
    )(reply, tail_out, tail_stat)


def solution(mesh):
    sizes = mesh.shape
    names = [n for a in mesh.axis_names for n in (RING if a == "ctx" else (a,))]
    ring = sizes["ctx"]
    lengths = {**sizes, "hi": ring // NEAR, "lo": NEAR}
    split = jax.sharding.Mesh(mesh.devices.reshape([lengths[n] for n in names]), tuple(names))
    rows = ("groups",) + RING + ("row",)
    by_row = P(None, rows, "rep", None)
    by_page = P("rep", ("groups",) + RING, None)
    return jax.shard_map(
        functools.partial(per_device, ring),
        mesh=split,
        in_specs=(by_row,) * 3 + (by_page,) * 4 + (P("rep", "groups"), P(rows, "rep", None)),
        out_specs=by_row,
        check_vma=False,
    )
```

```python
import functools
import math

import jax
import jax.numpy as jnp
from jax import lax
from jax.experimental import pallas as pl
from jax.experimental.pallas import tpu as pltpu
from jax.sharding import PartitionSpec as P


FLOOR_SCORE = -10000.0
MASKED = -(2.0**100)
NEAR = 4
RING = ("hi", "lo")
PEERS = ("hi", "row")
LANES = 128
EXTRA = 2
SMALLEST = 2.0**-100
LOW_SCALE = 1024.0
LOG2_E = math.log2(math.e)
CHUNK = 256


def as_bf16(x):
    return x.astype(jnp.bfloat16).astype(jnp.float32)


def place():
    return lax.axis_index("hi") * NEAR + lax.axis_index("lo"), lax.axis_index("row")


def near_offsets(core):
    return (0, 1, -1, 2 - 4 * core)


def head_queries(q_ref, heads, head):
    num_steps, _, num_heads, _ = q_ref.shape
    group = num_heads // heads
    rows = slice(head * group, (head + 1) * group)
    return [q_ref[s, 0, rows, :].astype(jnp.float32) for s in range(num_steps)]


def prepare(
    heads, picks_ref, slots_ref, q_hbm, k_ref, v_ref, ck_ref, cv_ref, pages_ref, ask_ref,
    q_ref, ck_own, cv_own, arrived,
):
    core = lax.axis_index("row")
    span, width = k_ref.shape[1:]
    near = ck_ref.shape[1]
    moves = (
        (q_hbm, q_ref),
        (ck_ref.at[core], ck_own),
        (cv_ref.at[core], cv_own),
        (k_ref.at[core], pages_ref.at[pl.ds(0, span)]),
        (v_ref.at[core], pages_ref.at[pl.ds(span, span)]),
    )
    copies = [pltpu.make_async_copy(*move, arrived.at[i]) for i, move in enumerate(moves)]
    for copy in copies:
        copy.start()
    lane = lax.broadcasted_iota(jnp.int32, (8, width), 1)
    sub = lax.broadcasted_iota(jnp.int32, (8, width), 0)
    masks = []
    for head in range(heads):
        slot_free = jnp.ones((8, width), jnp.float32)
        cluster_used = jnp.zeros((8, width), jnp.float32)
        for i in range(picks_ref.shape[2]):
            pick = picks_ref[0, head, i]
            slot_free = jnp.where(lane == slots_ref[head, pick], 0.0, slot_free)
            cluster_used = jnp.where(lane == pick, 1.0, cluster_used)
        masks.append(jnp.where(sub == 0, slot_free, jnp.where(sub == 1, cluster_used, 0.0)))
    copies[0].wait()
    for head in range(heads):
        message = jnp.concatenate(head_queries(q_ref, heads, head) + [masks[head]], axis=0)
        height = message.shape[0] - 8 + EXTRA
        message = message[0:height].astype(ask_ref.dtype)
        for peer in range(head, ask_ref.shape[0] // height, heads):
            ask_ref[peer * height : (peer + 1) * height, :] = message
    for copy in copies[1:3]:
        copy.wait()
    coarse = jnp.concatenate(
        [ck_own[...].astype(jnp.float32), cv_own[...].astype(jnp.float32)]
        + [jnp.zeros((16 - 2 * near, width), jnp.float32)],
        axis=0,
    )
    pages_ref[2 * span :, :] = coarse.astype(pages_ref.dtype)
    for copy in copies[3:]:
        copy.wait()


def tail(heads, q_ref, nk_ref, nv_ref, out_ref, stat_ref):
    num_steps, _, num_heads, width = q_ref.shape
    per_peer = num_steps * num_heads // heads
    scale = 1.0 / math.sqrt(width)
    step = lax.broadcasted_iota(jnp.int32, (per_peer, 1), 0) // (num_heads // heads)
    lane = lax.broadcasted_iota(jnp.int32, (per_peer, width), 1)
    for head in range(heads):
        queries = jnp.concatenate(head_queries(q_ref, heads, head), axis=0)
        scores = []
        for t in range(num_steps):
            key = nk_ref[t, 0, head : head + 1, :].astype(jnp.float32)
            scores.append(jnp.sum(queries * key, axis=1, keepdims=True) * scale)
        top = functools.reduce(
            jnp.maximum, [jnp.where(step >= t, scores[t], FLOOR_SCORE) for t in range(num_steps)]
        )
        total = jnp.zeros((per_peer, 1), jnp.float32)
        out = jnp.zeros((per_peer, width), jnp.float32)
        for t in range(num_steps):
            weight = jnp.where(step >= t, jnp.exp(jnp.minimum(scores[t] - top, 0.0)), 0.0)
            total += weight
            value = nv_ref[t, 0, head : head + 1, :].astype(jnp.float32)
            out += weight.astype(jnp.bfloat16).astype(jnp.float32) * value
        out_ref[head] = out
        stat_ref[head] = jnp.where(lane == 0, top, total)


def arrange(span, near, ring, *refs):
    page_refs, (keys_ref, values_ref, ends_ref, end_values_ref) = refs[:NEAR], refs[NEAR:]
    width = page_refs[0].shape[1]
    position, core = place()
    shards = [lax.rem(position + off + ring, ring) for off in near_offsets(core)]
    page = span // near
    lane = lax.broadcasted_iota(jnp.int32, (page, width), 1)
    row = lax.broadcasted_iota(jnp.int32, (NEAR * near, width), 0)
    column = lax.broadcasted_iota(jnp.int32, (NEAR * near, width), 1)
    cluster = jnp.full((NEAR * near, width), -1, jnp.int32)
    for b, (ref, shard) in enumerate(zip(page_refs, shards)):
        keys_ref[b, :, 0:width] = ref[0:span, :]
        for p in range(near):
            picker = jnp.where(lane == shard * near + p, MASKED, 0.0)
            keys_ref[b, p * page : (p + 1) * page, width:] = picker.astype(jnp.bfloat16)
        values_ref[b] = jnp.transpose(ref[span : 2 * span, :])
        cluster = jnp.where(row // near == b, shard * near + row - b * near, cluster)
    ends = [ref[2 * span :, :].astype(jnp.float32) for ref in page_refs]
    picker = jnp.where(column == cluster, MASKED, 0.0)
    coarse = jnp.concatenate([e[0:near] for e in ends], axis=0)
    ends_ref[...] = jnp.concatenate([coarse, picker], axis=1).astype(jnp.bfloat16)
    blank = jnp.zeros((LANES - near * NEAR, width), jnp.float32)
    coarse = jnp.concatenate([e[near : 2 * near] for e in ends] + [blank], axis=0)
    end_values_ref[...] = jnp.transpose(coarse)[:, 0 : near * NEAR].astype(jnp.bfloat16)


def attend(span, near, peers, ask_ref, keys_ref, values_ref, ends_ref, end_values_ref, reply_ref):
    width = ask_ref.shape[1]
    height = ask_ref.shape[0] // peers
    per_peer = height - EXTRA
    scale = LOG2_E / math.sqrt(width)
    log_page = math.log2(span // near)
    floor = FLOOR_SCORE * LOG2_E
    chunk_peers = CHUNK // per_peer
    parts = LANES // per_peer
    contract_last = (((1,), (1,)), ((), ()))
    block_of = lax.broadcasted_iota(jnp.int32, (NEAR * near, CHUNK), 0) // near
    part_of = lax.broadcasted_iota(jnp.int32, (EXTRA, LANES), 1) // per_peer
    sub = lax.broadcasted_iota(jnp.int32, (8, CHUNK), 0)
    ends = ends_ref[...]
    end_values = end_values_ref[...]

    for chunk in range(peers // chunk_peers):
        first = chunk * chunk_peers * height
        asked = ask_ref[first : first + chunk_peers * height, :].astype(jnp.float32)
        asked = [asked[i * height : (i + 1) * height] for i in range(chunk_peers)]
        queries = jnp.concatenate([a[:per_peer] for a in asked], axis=0).astype(jnp.bfloat16)
        spread = lambda i: jnp.concatenate(
            [jnp.broadcast_to(a[per_peer + i :][0:1], (per_peer, width)) for a in asked], axis=0
        ).astype(jnp.bfloat16)
        exact_queries = jnp.concatenate([queries, spread(0)], axis=1)
        coarse_queries = jnp.concatenate([queries, spread(1)], axis=1)
        coarse = lax.dot_general(
            ends, coarse_queries, contract_last, preferred_element_type=jnp.float32
        )
        coarse = coarse * scale + log_page
        tops, totals, outs = [], [], []
        for b in range(NEAR):
            scores = lax.dot_general(
                keys_ref[b], exact_queries, contract_last, preferred_element_type=jnp.float32
            )
            mine = block_of == b
            top = jnp.maximum(
                jnp.max(scores, axis=0, keepdims=True) * scale,
                jnp.max(jnp.where(mine, coarse, floor), axis=0, keepdims=True),
            )
            top = jnp.maximum(top, floor)
            weights = jnp.exp2(scores * scale - top)
            coarse_weights = jnp.where(mine, jnp.exp2(jnp.where(mine, coarse - top, 0.0)), 0.0)
            totals.append(
                jnp.sum(weights, axis=0, keepdims=True)
                + jnp.sum(coarse_weights, axis=0, keepdims=True)
            )
            outs.append(
                jnp.dot(
                    values_ref[b],
                    weights.astype(jnp.bfloat16),
                    preferred_element_type=jnp.float32,
                )
                + jnp.dot(
                    end_values,
                    coarse_weights.astype(jnp.bfloat16),
                    preferred_element_type=jnp.float32,
                )
            )
            tops.append(top)
        best = functools.reduce(jnp.maximum, tops)
        factors = [jnp.exp2(t - best) for t in tops]
        total = sum(f * t for f, t in zip(factors, totals))
        out = sum(f * o for f, o in zip(factors, outs))
        some = total > 0.0
        level = jnp.where(some, best + jnp.log2(jnp.where(some, total, 1.0)), 2 * floor)
        out = out * jnp.where(some, 1.0 / jnp.where(some, total, 1.0), 0.0)
        largest = jnp.max(jnp.abs(out), axis=0, keepdims=True)
        power = jnp.ceil(jnp.log2(jnp.maximum(largest, SMALLEST)))
        out = jnp.transpose(out * jnp.exp2(-power))
        high = as_bf16(level)
        middle = as_bf16(level - high)
        low = (level - high - middle) * LOW_SCALE
        stats = jnp.zeros((8, CHUNK), jnp.float32)
        for i, part in enumerate((high, middle, low, power)):
            stats = jnp.where(sub == i, part, stats)
        for half in range(CHUNK // LANES):
            held = stats[:, half * LANES : (half + 1) * LANES]
            turns = [pltpu.roll(held, i * per_peer, 1) if i else held for i in range(parts)]
            for i in range(parts):
                peer = half * parts + i
                at = first + peer * height
                reply_ref[at : at + per_peer, :] = out[peer * per_peer : (peer + 1) * per_peer]
                line = jnp.zeros((EXTRA, LANES), jnp.float32)
                for part in range(parts):
                    turned = turns[(part - i) % parts][part : part + 1]
                    line = jnp.where(part_of == part, turned, line)
                reply_ref[at + per_peer : at + height, :] = line


def merge(heads, peers, reply_ref, tail_ref, tail_stat_ref, o_ref):
    num_steps, _, num_heads, _ = o_ref.shape
    group = num_heads // heads
    height = reply_ref.shape[0] // peers
    per_peer = height - EXTRA
    replies = [reply_ref[p * height : (p + 1) * height, :] for p in range(peers)]
    stats = [r[per_peer : per_peer + 1] for r in replies]
    stats = jnp.transpose(
        jnp.concatenate(stats + [jnp.zeros((LANES - peers, LANES), jnp.float32)], axis=0)
    )
    high, middle, low, power = (stats[i * per_peer : (i + 1) * per_peer] for i in range(4))
    levels = high + (middle + low * (1.0 / LOW_SCALE))
    powers = jnp.exp2(power)
    results = []
    for head in range(heads):
        sources = range(head, peers, heads)
        tops = [levels[:, p : p + 1] for p in sources]
        tail_top = tail_stat_ref[head, :, 0:1] * LOG2_E
        best = functools.reduce(jnp.maximum, tops, tail_top)
        factor = jnp.exp2(tail_top - best)
        numer, denom = factor * tail_ref[head], factor * tail_stat_ref[head, :, 1:2]
        for p, top in zip(sources, tops):
            factor = jnp.exp2(top - best)
            numer += (factor * powers[:, p : p + 1]) * replies[p][0:per_peer]
            denom += factor
        results.append(numer / denom)
    for s in range(num_steps):
        rows = [r[s * group : (s + 1) * group] for r in results]
        o_ref[s, 0] = jnp.concatenate(rows, axis=0).astype(o_ref.dtype)


VMEM = pl.BlockSpec(memory_space=pltpu.VMEM)
SMEM = pl.BlockSpec(memory_space=pltpu.SMEM)
HBM = pl.BlockSpec(memory_space=pltpu.HBM)


def on_core(kernel, out_shape, in_specs, flops, mib, scratch=()):
    many = isinstance(out_shape, tuple)
    return pl.pallas_call(
        kernel,
        out_shape=out_shape,
        in_specs=in_specs,
        out_specs=(VMEM,) * len(out_shape) if many else VMEM,
        scratch_shapes=scratch,
        cost_estimate=pl.CostEstimate(flops=flops, bytes_accessed=2**20, transcendentals=0),
        compiler_params=pltpu.CompilerParams(vmem_limit_bytes=mib * 2**20),
    )


def exchange(messages, peers):
    pairs = messages.reshape(peers, -1, 2, messages.shape[1])
    return lax.all_to_all(pairs, PEERS, 0, 0, tiled=True).reshape(messages.shape)


def per_device(ring, queries, new_keys, step_new_values, keys, values, cent_keys, cent_values, slots, picks):
    num_steps, _, num_heads, width = queries.shape
    heads, span = keys.shape[:2]
    near = cent_keys.shape[1]
    cores = lax.axis_size("row")
    peers = lax.axis_size("hi") * cores
    per_peer = num_steps * num_heads // heads
    height = per_peer + EXTRA
    shape = jax.ShapeDtypeStruct
    pages, ask = on_core(
        functools.partial(prepare, heads),
        (
            shape((2 * span + 16, width), jnp.bfloat16),
            shape((peers * height, width), jnp.bfloat16),
        ),
        [SMEM] * 2 + [HBM] * 5,
        2**16,
        60,
        [pltpu.VMEM(queries.shape, jnp.bfloat16)]
        + [pltpu.VMEM((near, width), jnp.bfloat16)] * 2
        + [pltpu.SemaphoreType.DMA((5,))],
    )(picks, slots, queries, keys, values, cent_keys, cent_values)
    every = [(z, c) for z in range(ring) for c in range(cores)]
    shift = lambda of: [(((z + of(c)) % ring) * cores + c, z * cores + c) for z, c in every]
    fetched = [pages]
    for i in range(1, NEAR):
        pairs = shift(lambda c: near_offsets(c)[i])
        fetched.append(lax.ppermute(pages, RING + ("row",), pairs))
    asked = exchange(ask, peers)
    tail_out, tail_stat = on_core(
        functools.partial(tail, heads),
        (shape((heads, per_peer, width), jnp.float32),) * 2,
        [VMEM] * 3,
        2**22,
        4,
    )(queries, new_keys, step_new_values)
    arranged = on_core(
        functools.partial(arrange, span, near, ring),
        (
            shape((NEAR, span, 2 * width), jnp.bfloat16),
            shape((NEAR, width, span), jnp.bfloat16),
            shape((NEAR * near, 2 * width), jnp.bfloat16),
            shape((width, NEAR * near), jnp.bfloat16),
        ),
        [VMEM] * NEAR,
        2**22,
        20,
    )(*fetched)
    reply = on_core(
        functools.partial(attend, span, near, peers),
        shape((peers * height, width), jnp.float32),
        [VMEM] * 5,
        4 * peers * per_peer * span * NEAR * width,
        20,
    )(asked, *arranged)
    reply = exchange(reply.astype(jnp.float16), peers).astype(jnp.float32)
    return on_core(
        functools.partial(merge, heads, peers),
        shape(queries.shape, jnp.bfloat16),
        [VMEM] * 3,
        2**20,
        8,
    )(reply, tail_out, tail_stat)


def solution(mesh):
    sizes = mesh.shape
    names = [n for a in mesh.axis_names for n in (RING if a == "ctx" else (a,))]
    ring = sizes["ctx"]
    lengths = {**sizes, "hi": ring // NEAR, "lo": NEAR}
    split = jax.sharding.Mesh(mesh.devices.reshape([lengths[n] for n in names]), tuple(names))
    rows = ("groups",) + RING + ("row",)
    by_row = P(None, rows, "rep", None)
    by_page = P("rep", ("groups",) + RING, None)
    return jax.shard_map(
        functools.partial(per_device, ring),
        mesh=split,
        in_specs=(by_row,) * 3 + (by_page,) * 4 + (P("rep", "groups"), P(rows, "rep", None)),
        out_specs=by_row,
        check_vma=False,
    )
```

```python
import functools
import math

import jax
import jax.numpy as jnp
from jax import lax
from jax.experimental import pallas as pl
from jax.experimental.pallas import tpu as pltpu
from jax.sharding import PartitionSpec as P


FLOOR_SCORE = -10000.0
MASKED = -(2.0**100)
NEAR = 4
RING = ("hi", "lo")
PEERS = ("hi", "row")
LANES = 128
EXTRA = 2
SMALLEST = 2.0**-100
LOW_SCALE = 1024.0
LOG2_E = math.log2(math.e)
CHUNK = 256


def as_bf16(x):
    return x.astype(jnp.bfloat16).astype(jnp.float32)


def place():
    return lax.axis_index("hi") * NEAR + lax.axis_index("lo"), lax.axis_index("row")


def near_offsets(core):
    return (0, 1, -1, 2 - 4 * core)


def head_queries(q_ref, heads, head):
    num_steps, _, num_heads, _ = q_ref.shape
    group = num_heads // heads
    rows = slice(head * group, (head + 1) * group)
    return [q_ref[s, 0, rows, :].astype(jnp.float32) for s in range(num_steps)]


def prepare(
    heads, picks_hbm, slots_hbm, q_hbm, k_ref, v_ref, ck_ref, cv_ref, pages_ref, ask_ref,
    picks_ref, slots_ref, q_ref, ck_own, cv_own, arrived,
):
    core = lax.axis_index("row")
    span, width = k_ref.shape[1:]
    near = ck_ref.shape[1]
    moves = (
        (picks_hbm, picks_ref),
        (slots_hbm, slots_ref),
        (q_hbm, q_ref),
        (ck_ref.at[core], ck_own),
        (cv_ref.at[core], cv_own),
        (k_ref.at[core], pages_ref.at[pl.ds(0, span)]),
        (v_ref.at[core], pages_ref.at[pl.ds(span, span)]),
    )
    copies = [pltpu.make_async_copy(*move, arrived.at[i]) for i, move in enumerate(moves)]
    for copy in copies:
        copy.start()
    lane = lax.broadcasted_iota(jnp.int32, (8, width), 1)
    sub = lax.broadcasted_iota(jnp.int32, (8, width), 0)
    masks = []
    for copy in copies[:2]:
        copy.wait()
    for head in range(heads):
        slot_free = jnp.ones((8, width), jnp.float32)
        cluster_used = jnp.zeros((8, width), jnp.float32)
        for i in range(picks_ref.shape[2]):
            pick = picks_ref[0, head, i]
            slot_free = jnp.where(lane == slots_ref[head, pick], 0.0, slot_free)
            cluster_used = jnp.where(lane == pick, 1.0, cluster_used)
        masks.append(jnp.where(sub == 0, slot_free, jnp.where(sub == 1, cluster_used, 0.0)))
    copies[2].wait()
    for head in range(heads):
        message = jnp.concatenate(head_queries(q_ref, heads, head) + [masks[head]], axis=0)
        height = message.shape[0] - 8 + EXTRA
        message = message[0:height].astype(ask_ref.dtype)
        for peer in range(head, ask_ref.shape[0] // height, heads):
            ask_ref[peer * height : (peer + 1) * height, :] = message
    for copy in copies[3:5]:
        copy.wait()
    coarse = jnp.concatenate(
        [ck_own[...].astype(jnp.float32), cv_own[...].astype(jnp.float32)]
        + [jnp.zeros((16 - 2 * near, width), jnp.float32)],
        axis=0,
    )
    pages_ref[2 * span :, :] = coarse.astype(pages_ref.dtype)
    for copy in copies[5:]:
        copy.wait()


def tail(heads, q_ref, nk_ref, nv_ref, out_ref, stat_ref):
    num_steps, _, num_heads, width = q_ref.shape
    per_peer = num_steps * num_heads // heads
    scale = 1.0 / math.sqrt(width)
    step = lax.broadcasted_iota(jnp.int32, (per_peer, 1), 0) // (num_heads // heads)
    lane = lax.broadcasted_iota(jnp.int32, (per_peer, width), 1)
    for head in range(heads):
        queries = jnp.concatenate(head_queries(q_ref, heads, head), axis=0)
        scores = []
        for t in range(num_steps):
            key = nk_ref[t, 0, head : head + 1, :].astype(jnp.float32)
            scores.append(jnp.sum(queries * key, axis=1, keepdims=True) * scale)
        top = functools.reduce(
            jnp.maximum, [jnp.where(step >= t, scores[t], FLOOR_SCORE) for t in range(num_steps)]
        )
        total = jnp.zeros((per_peer, 1), jnp.float32)
        out = jnp.zeros((per_peer, width), jnp.float32)
        for t in range(num_steps):
            weight = jnp.where(step >= t, jnp.exp(jnp.minimum(scores[t] - top, 0.0)), 0.0)
            total += weight
            value = nv_ref[t, 0, head : head + 1, :].astype(jnp.float32)
            out += weight.astype(jnp.bfloat16).astype(jnp.float32) * value
        out_ref[head] = out
        stat_ref[head] = jnp.where(lane == 0, top, total)


def arrange(span, near, ring, *refs):
    page_refs, (keys_ref, values_ref, ends_ref, end_values_ref) = refs[:NEAR], refs[NEAR:]
    width = page_refs[0].shape[1]
    position, core = place()
    shards = [lax.rem(position + off + ring, ring) for off in near_offsets(core)]
    page = span // near
    lane = lax.broadcasted_iota(jnp.int32, (page, width), 1)
    row = lax.broadcasted_iota(jnp.int32, (NEAR * near, width), 0)
    column = lax.broadcasted_iota(jnp.int32, (NEAR * near, width), 1)
    cluster = jnp.full((NEAR * near, width), -1, jnp.int32)
    for b, (ref, shard) in enumerate(zip(page_refs, shards)):
        keys_ref[b, :, 0:width] = ref[0:span, :]
        for p in range(near):
            picker = jnp.where(lane == shard * near + p, MASKED, 0.0)
            keys_ref[b, p * page : (p + 1) * page, width:] = picker.astype(jnp.bfloat16)
        values_ref[b] = jnp.transpose(ref[span : 2 * span, :])
        cluster = jnp.where(row // near == b, shard * near + row - b * near, cluster)
    ends = [ref[2 * span :, :].astype(jnp.float32) for ref in page_refs]
    picker = jnp.where(column == cluster, MASKED, 0.0)
    coarse = jnp.concatenate([e[0:near] for e in ends], axis=0)
    ends_ref[...] = jnp.concatenate([coarse, picker], axis=1).astype(jnp.bfloat16)
    blank = jnp.zeros((LANES - near * NEAR, width), jnp.float32)
    coarse = jnp.concatenate([e[near : 2 * near] for e in ends] + [blank], axis=0)
    end_values_ref[...] = jnp.transpose(coarse)[:, 0 : near * NEAR].astype(jnp.bfloat16)


def attend(span, near, peers, ask_ref, keys_ref, values_ref, ends_ref, end_values_ref, reply_ref):
    width = ask_ref.shape[1]
    height = ask_ref.shape[0] // peers
    per_peer = height - EXTRA
    scale = LOG2_E / math.sqrt(width)
    log_page = math.log2(span // near)
    floor = FLOOR_SCORE * LOG2_E
    chunk_peers = CHUNK // per_peer
    parts = LANES // per_peer
    contract_last = (((1,), (1,)), ((), ()))
    block_of = lax.broadcasted_iota(jnp.int32, (NEAR * near, CHUNK), 0) // near
    part_of = lax.broadcasted_iota(jnp.int32, (EXTRA, LANES), 1) // per_peer
    sub = lax.broadcasted_iota(jnp.int32, (8, CHUNK), 0)
    ends = ends_ref[...]
    end_values = end_values_ref[...]

    for chunk in range(peers // chunk_peers):
        first = chunk * chunk_peers * height
        asked = ask_ref[first : first + chunk_peers * height, :].astype(jnp.float32)
        asked = [asked[i * height : (i + 1) * height] for i in range(chunk_peers)]
        queries = jnp.concatenate([a[:per_peer] for a in asked], axis=0).astype(jnp.bfloat16)
        spread = lambda i: jnp.concatenate(
            [jnp.broadcast_to(a[per_peer + i :][0:1], (per_peer, width)) for a in asked], axis=0
        ).astype(jnp.bfloat16)
        exact_queries = jnp.concatenate([queries, spread(0)], axis=1)
        coarse_queries = jnp.concatenate([queries, spread(1)], axis=1)
        coarse = lax.dot_general(
            ends, coarse_queries, contract_last, preferred_element_type=jnp.float32
        )
        coarse = coarse * scale + log_page
        tops, totals, outs = [], [], []
        for b in range(NEAR):
            scores = lax.dot_general(
                keys_ref[b], exact_queries, contract_last, preferred_element_type=jnp.float32
            )
            mine = block_of == b
            top = jnp.maximum(
                jnp.max(scores, axis=0, keepdims=True) * scale,
                jnp.max(jnp.where(mine, coarse, floor), axis=0, keepdims=True),
            )
            top = jnp.maximum(top, floor)
            weights = jnp.exp2(scores * scale - top)
            coarse_weights = jnp.where(mine, jnp.exp2(jnp.where(mine, coarse - top, 0.0)), 0.0)
            totals.append(
                jnp.sum(weights, axis=0, keepdims=True)
                + jnp.sum(coarse_weights, axis=0, keepdims=True)
            )
            outs.append(
                jnp.dot(
                    values_ref[b],
                    weights.astype(jnp.bfloat16),
                    preferred_element_type=jnp.float32,
                )
                + jnp.dot(
                    end_values,
                    coarse_weights.astype(jnp.bfloat16),
                    preferred_element_type=jnp.float32,
                )
            )
            tops.append(top)
        best = functools.reduce(jnp.maximum, tops)
        factors = [jnp.exp2(t - best) for t in tops]
        total = sum(f * t for f, t in zip(factors, totals))
        out = sum(f * o for f, o in zip(factors, outs))
        some = total > 0.0
        level = jnp.where(some, best + jnp.log2(jnp.where(some, total, 1.0)), 2 * floor)
        out = out * jnp.where(some, 1.0 / jnp.where(some, total, 1.0), 0.0)
        largest = jnp.max(jnp.abs(out), axis=0, keepdims=True)
        power = jnp.ceil(jnp.log2(jnp.maximum(largest, SMALLEST)))
        out = jnp.transpose(out * jnp.exp2(-power))
        high = as_bf16(level)
        middle = as_bf16(level - high)
        low = (level - high - middle) * LOW_SCALE
        stats = jnp.zeros((8, CHUNK), jnp.float32)
        for i, part in enumerate((high, middle, low, power)):
            stats = jnp.where(sub == i, part, stats)
        for half in range(CHUNK // LANES):
            held = stats[:, half * LANES : (half + 1) * LANES]
            turns = [pltpu.roll(held, i * per_peer, 1) if i else held for i in range(parts)]
            for i in range(parts):
                peer = half * parts + i
                at = first + peer * height
                reply_ref[at : at + per_peer, :] = out[peer * per_peer : (peer + 1) * per_peer]
                line = jnp.zeros((EXTRA, LANES), jnp.float32)
                for part in range(parts):
                    turned = turns[(part - i) % parts][part : part + 1]
                    line = jnp.where(part_of == part, turned, line)
                reply_ref[at + per_peer : at + height, :] = line


def merge(heads, peers, reply_ref, tail_ref, tail_stat_ref, o_ref):
    num_steps, _, num_heads, _ = o_ref.shape
    group = num_heads // heads
    height = reply_ref.shape[0] // peers
    per_peer = height - EXTRA
    replies = [reply_ref[p * height : (p + 1) * height, :] for p in range(peers)]
    stats = [r[per_peer : per_peer + 1] for r in replies]
    stats = jnp.transpose(
        jnp.concatenate(stats + [jnp.zeros((LANES - peers, LANES), jnp.float32)], axis=0)
    )
    high, middle, low, power = (stats[i * per_peer : (i + 1) * per_peer] for i in range(4))
    levels = high + (middle + low * (1.0 / LOW_SCALE))
    powers = jnp.exp2(power)
    results = []
    for head in range(heads):
        sources = range(head, peers, heads)
        tops = [levels[:, p : p + 1] for p in sources]
        tail_top = tail_stat_ref[head, :, 0:1] * LOG2_E
        best = functools.reduce(jnp.maximum, tops, tail_top)
        factor = jnp.exp2(tail_top - best)
        numer, denom = factor * tail_ref[head], factor * tail_stat_ref[head, :, 1:2]
        for p, top in zip(sources, tops):
            factor = jnp.exp2(top - best)
            numer += (factor * powers[:, p : p + 1]) * replies[p][0:per_peer]
            denom += factor
        results.append(numer / denom)
    for s in range(num_steps):
        rows = [r[s * group : (s + 1) * group] for r in results]
        o_ref[s, 0] = jnp.concatenate(rows, axis=0).astype(o_ref.dtype)


VMEM = pl.BlockSpec(memory_space=pltpu.VMEM)
HBM = pl.BlockSpec(memory_space=pltpu.HBM)


def on_core(kernel, out_shape, in_specs, flops, mib, scratch=()):
    many = isinstance(out_shape, tuple)
    return pl.pallas_call(
        kernel,
        out_shape=out_shape,
        in_specs=in_specs,
        out_specs=(VMEM,) * len(out_shape) if many else VMEM,
        scratch_shapes=scratch,
        cost_estimate=pl.CostEstimate(flops=flops, bytes_accessed=2**20, transcendentals=0),
        compiler_params=pltpu.CompilerParams(vmem_limit_bytes=mib * 2**20),
    )


def exchange(messages, peers):
    pairs = messages.reshape(peers, -1, 2, messages.shape[1])
    return lax.all_to_all(pairs, PEERS, 0, 0, tiled=True).reshape(messages.shape)


def per_device(ring, queries, new_keys, step_new_values, keys, values, cent_keys, cent_values, slots, picks):
    num_steps, _, num_heads, width = queries.shape
    heads, span = keys.shape[:2]
    near = cent_keys.shape[1]
    cores = lax.axis_size("row")
    peers = lax.axis_size("hi") * cores
    per_peer = num_steps * num_heads // heads
    height = per_peer + EXTRA
    shape = jax.ShapeDtypeStruct
    pages, ask = on_core(
        functools.partial(prepare, heads),
        (
            shape((2 * span + 16, width), jnp.bfloat16),
            shape((peers * height, width), jnp.bfloat16),
        ),
        [HBM] * 7,
        2**16,
        60,
        [pltpu.SMEM(picks.shape, jnp.int32), pltpu.SMEM(slots.shape, jnp.int32)]
        + [pltpu.VMEM(queries.shape, jnp.bfloat16)]
        + [pltpu.VMEM((near, width), jnp.bfloat16)] * 2
        + [pltpu.SemaphoreType.DMA((7,))],
    )(picks, slots, queries, keys, values, cent_keys, cent_values)
    every = [(z, c) for z in range(ring) for c in range(cores)]
    shift = lambda of: [(((z + of(c)) % ring) * cores + c, z * cores + c) for z, c in every]
    fetched = [pages]
    for i in range(1, NEAR):
        pairs = shift(lambda c: near_offsets(c)[i])
        fetched.append(lax.ppermute(pages, RING + ("row",), pairs))
    asked = exchange(ask, peers)
    tail_out, tail_stat = on_core(
        functools.partial(tail, heads),
        (shape((heads, per_peer, width), jnp.float32),) * 2,
        [VMEM] * 3,
        2**22,
        4,
    )(queries, new_keys, step_new_values)
    arranged = on_core(
        functools.partial(arrange, span, near, ring),
        (
            shape((NEAR, span, 2 * width), jnp.bfloat16),
            shape((NEAR, width, span), jnp.bfloat16),
            shape((NEAR * near, 2 * width), jnp.bfloat16),
            shape((width, NEAR * near), jnp.bfloat16),
        ),
        [VMEM] * NEAR,
        2**22,
        20,
    )(*fetched)
    reply = on_core(
        functools.partial(attend, span, near, peers),
        shape((peers * height, width), jnp.float32),
        [VMEM] * 5,
        4 * peers * per_peer * span * NEAR * width,
        20,
    )(asked, *arranged)
    reply = exchange(reply.astype(jnp.float16), peers).astype(jnp.float32)
    return on_core(
        functools.partial(merge, heads, peers),
        shape(queries.shape, jnp.bfloat16),
        [VMEM] * 3,
        2**20,
        8,
    )(reply, tail_out, tail_stat)


def solution(mesh):
    sizes = mesh.shape
    names = [n for a in mesh.axis_names for n in (RING if a == "ctx" else (a,))]
    ring = sizes["ctx"]
    lengths = {**sizes, "hi": ring // NEAR, "lo": NEAR}
    split = jax.sharding.Mesh(mesh.devices.reshape([lengths[n] for n in names]), tuple(names))
    rows = ("groups",) + RING + ("row",)
    by_row = P(None, rows, "rep", None)
    by_page = P("rep", ("groups",) + RING, None)
    return jax.shard_map(
        functools.partial(per_device, ring),
        mesh=split,
        in_specs=(by_row,) * 3 + (by_page,) * 4 + (P("rep", "groups"), P(rows, "rep", None)),
        out_specs=by_row,
        check_vma=False,
    )
```

```python
import functools
import math

import jax
import jax.numpy as jnp
from jax import lax
from jax.experimental import pallas as pl
from jax.experimental.pallas import tpu as pltpu
from jax.sharding import PartitionSpec as P


FLOOR_SCORE = -10000.0
MASKED = -(2.0**100)
NEAR = 4
RING = ("hi", "lo")
PEERS = ("hi", "row")
LANES = 128
EXTRA = 2
SMALLEST = 2.0**-100
LOW_SCALE = 1024.0
LOG2_E = math.log2(math.e)
CHUNK = 256


def as_bf16(x):
    return x.astype(jnp.bfloat16).astype(jnp.float32)


def place():
    return lax.axis_index("hi") * NEAR + lax.axis_index("lo"), lax.axis_index("row")


def near_offsets(core):
    return (0, 1 - 2 * core, 2 * core - 1, 2 - 4 * core)


def head_queries(q_ref, heads, head):
    num_steps, _, num_heads, _ = q_ref.shape
    group = num_heads // heads
    rows = slice(head * group, (head + 1) * group)
    return [q_ref[s, 0, rows, :].astype(jnp.float32) for s in range(num_steps)]


def prepare(
    heads, picks_hbm, slots_hbm, q_hbm, k_ref, v_ref, ck_ref, cv_ref, own_ref, both_ref, ask_ref,
    picks_ref, slots_ref, q_ref, ck_all, cv_all, arrived,
):
    core = lax.axis_index("row")
    span, width = k_ref.shape[1:]
    near = ck_ref.shape[1]
    size = own_ref.shape[0]
    places = ((core, own_ref, 0), (core, both_ref, 0), (1 - core, both_ref, size))
    moves = [
        (picks_hbm, picks_ref),
        (slots_hbm, slots_ref),
        (q_hbm, q_ref),
        (ck_ref, ck_all),
        (cv_ref, cv_all),
    ]
    for head, target, at in places:
        moves.append((k_ref.at[head], target.at[pl.ds(at, span)]))
        moves.append((v_ref.at[head], target.at[pl.ds(at + span, span)]))
    copies = [pltpu.make_async_copy(*move, arrived.at[i]) for i, move in enumerate(moves)]
    for copy in copies:
        copy.start()
    lane = lax.broadcasted_iota(jnp.int32, (8, width), 1)
    sub = lax.broadcasted_iota(jnp.int32, (8, width), 0)
    masks = []
    for copy in copies[:2]:
        copy.wait()
    for head in range(heads):
        slot_free = jnp.ones((8, width), jnp.float32)
        cluster_used = jnp.zeros((8, width), jnp.float32)
        for i in range(picks_ref.shape[2]):
            pick = picks_ref[0, head, i]
            slot_free = jnp.where(lane == slots_ref[head, pick], 0.0, slot_free)
            cluster_used = jnp.where(lane == pick, 1.0, cluster_used)
        masks.append(jnp.where(sub == 0, slot_free, jnp.where(sub == 1, cluster_used, 0.0)))
    copies[2].wait()
    for head in range(heads):
        message = jnp.concatenate(head_queries(q_ref, heads, head) + [masks[head]], axis=0)
        height = message.shape[0] - 8 + EXTRA
        message = message[0:height].astype(ask_ref.dtype)
        for peer in range(head, ask_ref.shape[0] // height, heads):
            ask_ref[peer * height : (peer + 1) * height, :] = message
    for copy in copies[3:5]:
        copy.wait()
    for head, target, at in places:
        coarse = jnp.concatenate(
            [ck_all[head].astype(jnp.float32), cv_all[head].astype(jnp.float32)]
            + [jnp.zeros((16 - 2 * near, width), jnp.float32)],
            axis=0,
        )
        target[at + 2 * span : at + size, :] = coarse.astype(target.dtype)
    for copy in copies[5:]:
        copy.wait()


def tail(heads, q_ref, nk_ref, nv_ref, out_ref, stat_ref):
    num_steps, _, num_heads, width = q_ref.shape
    per_peer = num_steps * num_heads // heads
    scale = 1.0 / math.sqrt(width)
    step = lax.broadcasted_iota(jnp.int32, (per_peer, 1), 0) // (num_heads // heads)
    lane = lax.broadcasted_iota(jnp.int32, (per_peer, width), 1)
    for head in range(heads):
        queries = jnp.concatenate(head_queries(q_ref, heads, head), axis=0)
        scores = []
        for t in range(num_steps):
            key = nk_ref[t, 0, head : head + 1, :].astype(jnp.float32)
            scores.append(jnp.sum(queries * key, axis=1, keepdims=True) * scale)
        top = functools.reduce(
            jnp.maximum, [jnp.where(step >= t, scores[t], FLOOR_SCORE) for t in range(num_steps)]
        )
        total = jnp.zeros((per_peer, 1), jnp.float32)
        out = jnp.zeros((per_peer, width), jnp.float32)
        for t in range(num_steps):
            weight = jnp.where(step >= t, jnp.exp(jnp.minimum(scores[t] - top, 0.0)), 0.0)
            total += weight
            value = nv_ref[t, 0, head : head + 1, :].astype(jnp.float32)
            out += weight.astype(jnp.bfloat16).astype(jnp.float32) * value
        out_ref[head] = out
        stat_ref[head] = jnp.where(lane == 0, top, total)


def arrange(span, near, ring, *refs):
    page_refs, (keys_ref, values_ref, ends_ref, end_values_ref) = refs[:NEAR], refs[NEAR:]
    size, width = page_refs[0].shape
    starts = (0, 0, size, 0)
    position, core = place()
    shards = [lax.rem(position + off + ring, ring) for off in near_offsets(core)]
    page = span // near
    lane = lax.broadcasted_iota(jnp.int32, (page, width), 1)
    row = lax.broadcasted_iota(jnp.int32, (NEAR * near, width), 0)
    column = lax.broadcasted_iota(jnp.int32, (NEAR * near, width), 1)
    cluster = jnp.full((NEAR * near, width), -1, jnp.int32)
    for b, (ref, shard, at) in enumerate(zip(page_refs, shards, starts)):
        keys_ref[b, :, 0:width] = ref[at : at + span, :]
        for p in range(near):
            picker = jnp.where(lane == shard * near + p, MASKED, 0.0)
            keys_ref[b, p * page : (p + 1) * page, width:] = picker.astype(jnp.bfloat16)
        values_ref[b] = jnp.transpose(ref[at + span : at + 2 * span, :])
        cluster = jnp.where(row // near == b, shard * near + row - b * near, cluster)
    ends = [
        ref[at + 2 * span : at + size, :].astype(jnp.float32)
        for ref, at in zip(page_refs, starts)
    ]
    picker = jnp.where(column == cluster, MASKED, 0.0)
    coarse = jnp.concatenate([e[0:near] for e in ends], axis=0)
    ends_ref[...] = jnp.concatenate([coarse, picker], axis=1).astype(jnp.bfloat16)
    blank = jnp.zeros((LANES - near * NEAR, width), jnp.float32)
    coarse = jnp.concatenate([e[near : 2 * near] for e in ends] + [blank], axis=0)
    end_values_ref[...] = jnp.transpose(coarse)[:, 0 : near * NEAR].astype(jnp.bfloat16)


def attend(span, near, peers, ask_ref, keys_ref, values_ref, ends_ref, end_values_ref, reply_ref):
    width = ask_ref.shape[1]
    height = ask_ref.shape[0] // peers
    per_peer = height - EXTRA
    scale = LOG2_E / math.sqrt(width)
    log_page = math.log2(span // near)
    floor = FLOOR_SCORE * LOG2_E
    chunk_peers = CHUNK // per_peer
    parts = LANES // per_peer
    contract_last = (((1,), (1,)), ((), ()))
    block_of = lax.broadcasted_iota(jnp.int32, (NEAR * near, CHUNK), 0) // near
    part_of = lax.broadcasted_iota(jnp.int32, (EXTRA, LANES), 1) // per_peer
    sub = lax.broadcasted_iota(jnp.int32, (8, CHUNK), 0)
    ends = ends_ref[...]
    end_values = end_values_ref[...]

    for chunk in range(peers // chunk_peers):
        first = chunk * chunk_peers * height
        asked = ask_ref[first : first + chunk_peers * height, :].astype(jnp.float32)
        asked = [asked[i * height : (i + 1) * height] for i in range(chunk_peers)]
        queries = jnp.concatenate([a[:per_peer] for a in asked], axis=0).astype(jnp.bfloat16)
        spread = lambda i: jnp.concatenate(
            [jnp.broadcast_to(a[per_peer + i :][0:1], (per_peer, width)) for a in asked], axis=0
        ).astype(jnp.bfloat16)
        exact_queries = jnp.concatenate([queries, spread(0)], axis=1)
        coarse_queries = jnp.concatenate([queries, spread(1)], axis=1)
        coarse = lax.dot_general(
            ends, coarse_queries, contract_last, preferred_element_type=jnp.float32
        )
        coarse = coarse * scale + log_page
        tops, totals, outs = [], [], []
        for b in range(NEAR):
            scores = lax.dot_general(
                keys_ref[b], exact_queries, contract_last, preferred_element_type=jnp.float32
            )
            mine = block_of == b
            top = jnp.maximum(
                jnp.max(scores, axis=0, keepdims=True) * scale,
                jnp.max(jnp.where(mine, coarse, floor), axis=0, keepdims=True),
            )
            top = jnp.maximum(top, floor)
            weights = jnp.exp2(scores * scale - top)
            coarse_weights = jnp.where(mine, jnp.exp2(jnp.where(mine, coarse - top, 0.0)), 0.0)
            totals.append(
                jnp.sum(weights, axis=0, keepdims=True)
                + jnp.sum(coarse_weights, axis=0, keepdims=True)
            )
            outs.append(
                jnp.dot(
                    values_ref[b],
                    weights.astype(jnp.bfloat16),
                    preferred_element_type=jnp.float32,
                )
                + jnp.dot(
                    end_values,
                    coarse_weights.astype(jnp.bfloat16),
                    preferred_element_type=jnp.float32,
                )
            )
            tops.append(top)
        best = functools.reduce(jnp.maximum, tops)
        factors = [jnp.exp2(t - best) for t in tops]
        total = sum(f * t for f, t in zip(factors, totals))
        out = sum(f * o for f, o in zip(factors, outs))
        some = total > 0.0
        level = jnp.where(some, best + jnp.log2(jnp.where(some, total, 1.0)), 2 * floor)
        out = out * jnp.where(some, 1.0 / jnp.where(some, total, 1.0), 0.0)
        largest = jnp.max(jnp.abs(out), axis=0, keepdims=True)
        power = jnp.ceil(jnp.log2(jnp.maximum(largest, SMALLEST)))
        out = jnp.transpose(out * jnp.exp2(-power))
        high = as_bf16(level)
        middle = as_bf16(level - high)
        low = (level - high - middle) * LOW_SCALE
        stats = jnp.zeros((8, CHUNK), jnp.float32)
        for i, part in enumerate((high, middle, low, power)):
            stats = jnp.where(sub == i, part, stats)
        for half in range(CHUNK // LANES):
            held = stats[:, half * LANES : (half + 1) * LANES]
            turns = [pltpu.roll(held, i * per_peer, 1) if i else held for i in range(parts)]
            for i in range(parts):
                peer = half * parts + i
                at = first + peer * height
                reply_ref[at : at + per_peer, :] = out[peer * per_peer : (peer + 1) * per_peer]
                line = jnp.zeros((EXTRA, LANES), jnp.float32)
                for part in range(parts):
                    turned = turns[(part - i) % parts][part : part + 1]
                    line = jnp.where(part_of == part, turned, line)
                reply_ref[at + per_peer : at + height, :] = line


def merge(heads, peers, reply_ref, tail_ref, tail_stat_ref, o_ref):
    num_steps, _, num_heads, _ = o_ref.shape
    group = num_heads // heads
    height = reply_ref.shape[0] // peers
    per_peer = height - EXTRA
    replies = [reply_ref[p * height : (p + 1) * height, :] for p in range(peers)]
    stats = [r[per_peer : per_peer + 1] for r in replies]
    stats = jnp.transpose(
        jnp.concatenate(stats + [jnp.zeros((LANES - peers, LANES), jnp.float32)], axis=0)
    )
    high, middle, low, power = (stats[i * per_peer : (i + 1) * per_peer] for i in range(4))
    levels = high + (middle + low * (1.0 / LOW_SCALE))
    powers = jnp.exp2(power)
    results = []
    for head in range(heads):
        sources = range(head, peers, heads)
        tops = [levels[:, p : p + 1] for p in sources]
        tail_top = tail_stat_ref[head, :, 0:1] * LOG2_E
        best = functools.reduce(jnp.maximum, tops, tail_top)
        factor = jnp.exp2(tail_top - best)
        numer, denom = factor * tail_ref[head], factor * tail_stat_ref[head, :, 1:2]
        for p, top in zip(sources, tops):
            factor = jnp.exp2(top - best)
            numer += (factor * powers[:, p : p + 1]) * replies[p][0:per_peer]
            denom += factor
        results.append(numer / denom)
    for s in range(num_steps):
        rows = [r[s * group : (s + 1) * group] for r in results]
        o_ref[s, 0] = jnp.concatenate(rows, axis=0).astype(o_ref.dtype)


VMEM = pl.BlockSpec(memory_space=pltpu.VMEM)
HBM = pl.BlockSpec(memory_space=pltpu.HBM)


def on_core(kernel, out_shape, in_specs, flops, mib, scratch=()):
    many = isinstance(out_shape, tuple)
    return pl.pallas_call(
        kernel,
        out_shape=out_shape,
        in_specs=in_specs,
        out_specs=(VMEM,) * len(out_shape) if many else VMEM,
        scratch_shapes=scratch,
        cost_estimate=pl.CostEstimate(flops=flops, bytes_accessed=2**20, transcendentals=0),
        compiler_params=pltpu.CompilerParams(vmem_limit_bytes=mib * 2**20),
    )


def exchange(messages, peers):
    pairs = messages.reshape(peers, -1, 2, messages.shape[1])
    return lax.all_to_all(pairs, PEERS, 0, 0, tiled=True).reshape(messages.shape)


def per_device(ring, queries, new_keys, step_new_values, keys, values, cent_keys, cent_values, slots, picks):
    num_steps, _, num_heads, width = queries.shape
    heads, span = keys.shape[:2]
    near = cent_keys.shape[1]
    cores = lax.axis_size("row")
    peers = lax.axis_size("hi") * cores
    per_peer = num_steps * num_heads // heads
    height = per_peer + EXTRA
    shape = jax.ShapeDtypeStruct
    size = 2 * span + 16
    own, both, ask = on_core(
        functools.partial(prepare, heads),
        (
            shape((size, width), jnp.bfloat16),
            shape((2 * size, width), jnp.bfloat16),
            shape((peers * height, width), jnp.bfloat16),
        ),
        [HBM] * 7,
        2**16,
        60,
        [pltpu.SMEM(picks.shape, jnp.int32), pltpu.SMEM(slots.shape, jnp.int32)]
        + [pltpu.VMEM(queries.shape, jnp.bfloat16)]
        + [pltpu.VMEM((heads, near, width), jnp.bfloat16)] * 2
        + [pltpu.SemaphoreType.DMA((11,))],
    )(picks, slots, queries, keys, values, cent_keys, cent_values)
    every = [(z, c) for z in range(ring) for c in range(cores)]

    def from_offset(pages, i):
        pairs = [
            (((z + near_offsets(c)[i]) % ring) * cores + c, z * cores + c) for z, c in every
        ]
        return lax.ppermute(pages, RING + ("row",), pairs)

    beside = from_offset(both, 1)
    beyond = from_offset(own, 3)
    swapped = lax.ppermute(beside, "row", [(0, 1), (1, 0)])
    fetched = (own, beside, swapped, beyond)
    asked = exchange(ask, peers)
    tail_out, tail_stat = on_core(
        functools.partial(tail, heads),
        (shape((heads, per_peer, width), jnp.float32),) * 2,
        [VMEM] * 3,
        2**22,
        4,
    )(queries, new_keys, step_new_values)
    arranged = on_core(
        functools.partial(arrange, span, near, ring),
        (
            shape((NEAR, span, 2 * width), jnp.bfloat16),
            shape((NEAR, width, span), jnp.bfloat16),
            shape((NEAR * near, 2 * width), jnp.bfloat16),
            shape((width, NEAR * near), jnp.bfloat16),
        ),
        [VMEM] * NEAR,
        2**22,
        20,
    )(*fetched)
    reply = on_core(
        functools.partial(attend, span, near, peers),
        shape((peers * height, width), jnp.float32),
        [VMEM] * 5,
        4 * peers * per_peer * span * NEAR * width,
        20,
    )(asked, *arranged)
    reply = exchange(reply.astype(jnp.float16), peers).astype(jnp.float32)
    return on_core(
        functools.partial(merge, heads, peers),
        shape(queries.shape, jnp.bfloat16),
        [VMEM] * 3,
        2**20,
        8,
    )(reply, tail_out, tail_stat)


def solution(mesh):
    sizes = mesh.shape
    names = [n for a in mesh.axis_names for n in (RING if a == "ctx" else (a,))]
    ring = sizes["ctx"]
    lengths = {**sizes, "hi": ring // NEAR, "lo": NEAR}
    split = jax.sharding.Mesh(mesh.devices.reshape([lengths[n] for n in names]), tuple(names))
    rows = ("groups",) + RING + ("row",)
    by_row = P(None, rows, "rep", None)
    by_page = P("rep", ("groups",) + RING, None)
    return jax.shard_map(
        functools.partial(per_device, ring),
        mesh=split,
        in_specs=(by_row,) * 3 + (by_page,) * 4 + (P("rep", "groups"), P(rows, "rep", None)),
        out_specs=by_row,
        check_vma=False,
    )
```
